32 devices in a mesh: dp: 1 (over z), col: 4 (over y), row: 8 (over x, core).
Axes of the slice: x: 4, y: 4, z: 1, core: 2. Of those that a mesh axis runs over, the one named last changes fastest.
The devices are a block of a 4x4x8 slice.
Arguments:
- x_act: bfloat16 [2048, 8192], P(('dp', 'row'), 'col')
- ln_gain: float32 [8192], P('col')
- w_in: bfloat16 [8192, 28672], P('row', 'col')
- w_out: bfloat16 [28672, 8192], P('row', 'col')
Outputs:
- output: bfloat16 [2048, 8192], P(('dp', 'row'), 'col')
All inputs are finite; a program needn't handle non-finite values.
Results may differ from the reference program's by a relative error of at most 0.00133.
Values are sent between devices in bfloat16 or wider.
A program may use at most 768 MiB of HBM per device.

```python
import jax
import jax.numpy as jnp
from jax import lax

TOKENS = 2048
D_MODEL = 8192
D_FF = 28672

NORM_EPS = 1e-5


def setup_inputs(seed: int = 0, part: int = 0) -> dict:
    key = jax.random.key(seed)
    part_key, shared_key = jax.random.split(key)
    part_key = jax.random.fold_in(part_key, part)
    key_noise, key_row, key_shift, key_scale = jax.random.split(part_key, 4)
    key_gain, key_in, key_out = jax.random.split(shared_key, 3)
    walk_norm = D_MODEL ** -0.5
    feat_shift = 0.8 * walk_norm * jnp.cumsum(jax.random.normal(key_shift, (D_MODEL,), jnp.float32))
    feat_scale = jnp.exp(0.5 * walk_norm * jnp.cumsum(jax.random.normal(key_scale, (D_MODEL,), jnp.float32)))
    row_shift = 0.5 * jax.random.normal(key_row, (TOKENS, 1), jnp.float32)
    noise = jax.random.normal(key_noise, (TOKENS, D_MODEL), jnp.float32)
    x_act = (noise * feat_scale + feat_shift + row_shift).astype(jnp.bfloat16)
    ln_gain = jax.random.uniform(key_gain, (D_MODEL,), jnp.float32, 0.5, 1.5)
    w_in = (D_MODEL ** -0.5 * jax.random.normal(key_in, (D_MODEL, D_FF), jnp.float32)).astype(jnp.bfloat16)
    w_out = (1.5 * D_FF ** -0.5 * jax.random.normal(key_out, (D_FF, D_MODEL), jnp.float32)).astype(jnp.bfloat16)
    return {"x_act": x_act, "ln_gain": ln_gain, "w_in": w_in, "w_out": w_out}


def reference(x_act, ln_gain, w_in, w_out):
    x_f32 = x_act.astype(jnp.float32)
    row_mean = jnp.mean(x_f32, axis=1, keepdims=True)
    row_var = jnp.mean(x_f32 * x_f32, axis=1, keepdims=True) - row_mean * row_mean
    z_norm = ((x_f32 - row_mean) * lax.rsqrt(row_var + NORM_EPS) * ln_gain).astype(jnp.bfloat16)
    hidden = jax.nn.gelu(jnp.dot(z_norm, w_in, preferred_element_type=jnp.float32), approximate=True).astype(jnp.bfloat16)
    branch = jnp.dot(hidden, w_out, preferred_element_type=jnp.float32)
    return (x_f32 + branch).astype(jnp.bfloat16)
```

```python
import functools

import jax
import jax.numpy as jnp
from jax import lax
from jax.experimental import pallas as pl
from jax.experimental.pallas import tpu as pltpu
from jax.sharding import PartitionSpec as P

NORM_EPS = 1e-5
MESH = pl.DeviceIdType.MESH
SUB = 4
LATE = 3


def gelu(v):
    return 0.5 * v * (1.0 + jnp.tanh(0.7978845608028654 * (v + 0.044715 * (v * v * v))))


class Sems:
    def __init__(self):
        self.base, self.total = {}, 0

    def add(self, name, count):
        self.base[name] = self.total
        self.total += count

    def __call__(self, name, index=0):
        return self.base[name] + index


def plan(tiles):
    s = Sems()
    for name, count in (
        ("stat", 3), ("zx", 4), ("zy", 16), ("w", 3 * tiles), ("wo", tiles), ("wf", 3 * tiles),
        ("wout", 1), ("h1a", 3), ("h1b", 3 * SUB), ("h2", 6 * SUB), ("ag", 8 * SUB), ("y", 3 * SUB),
    ):
        s.add(name, count)
    return s


def block(n, x_hbm, gain_ref, win, wout, y_hbm, w_hbm, wo_hbm, hst_a, hst_b, yr_hbm,
          xv, stat, z, wt, hm_a, hm_b, hf_a, hf_b, acc, wot, yt, ov, ss, rs, ls):
    nx, ny, d_model = n
    row, cy = lax.axis_index("row"), lax.axis_index("col")
    cx, k = row // 2, lax.rem(row, 2)
    tok, dloc = xv.shape
    tiles, krows, tw = w_hbm.shape[0], w_hbm.shape[2], w_hbm.shape[3]
    early = tiles - LATE
    half = tok // 2
    sub = tok // SUB
    sem = plan(tiles)

    def ring(v, d, m):
        return lax.rem(v + (d + m), m)

    def dev(dx=0, dy=0, core=None):
        return {"row": 2 * ring(cx, dx, nx) + (k if core is None else core), "col": ring(cy, dy, ny)}

    partner = dev(core=1 - k)

    def remote(src, dst, where, i):
        return pltpu.make_async_remote_copy(
            src_ref=src, dst_ref=dst, send_sem=ss.at[i], recv_sem=rs.at[i], device_id=where, device_id_type=MESH
        )

    sends, z_sends = [], []

    def send(src, dst, where, i, log=sends):
        c = remote(src, dst, where, i)
        c.start()
        log.append(c)

    def got(ref, i):
        remote(ref, ref, partner, i).wait_recv()

    load_x = pltpu.make_async_copy(x_hbm, xv, ls.at[0])
    load_x.start()
    barrier = pltpu.get_barrier_semaphore()
    peers = [partner] + [dev(dx=d) for d in range(1, nx)] + [dev(dy=d) for d in range(1, ny)]
    for p in peers:
        pl.semaphore_signal(barrier, inc=1, device_id=p, device_id_type=MESH)
    load_x.wait()

    lane = lax.broadcasted_iota(jnp.int32, stat.shape[1:], 1)

    def part(i, _):
        at = pl.ds(pl.multiple_of(i * 32, 32), 32)
        v = xv[at, :].astype(jnp.float32)
        s1 = jnp.sum(v, axis=1, keepdims=True)
        s2 = jnp.sum(v * v, axis=1, keepdims=True)
        stat[0, at, :] = jnp.where(lane[:32] == 0, s1, s2)
        return 0

    lax.fori_loop(0, tok // 32, part, 0)
    pl.semaphore_wait(barrier, len(peers))
    for d in range(1, ny):
        send(stat.at[0], stat.at[d], dev(dy=d), sem("stat", d - 1))

    def columns(dx, t):
        return pl.ds(pl.multiple_of(ring(cx, dx, nx) * (tiles * tw) + t * tw, 128), tw)

    def w_issue(t):
        for d in (1, 3, 2):
            send(win.at[:, columns(d, t)], w_hbm.at[t, row], dev(dx=d), sem("w", 3 * t + d - 1))
        send(win.at[:, columns(0, t)], w_hbm.at[t, row], partner, sem("wo", t))

    def w_forward(t):
        for d in (1, 3, 2):
            slot = 2 * ring(cx, -d, nx) + k
            got(w_hbm.at[t, slot], sem("w", 3 * t + d - 1))
            send(w_hbm.at[t, slot], w_hbm.at[t, slot], partner, sem("wf", 3 * t + d - 1))

    def w_ready(t):
        got(w_hbm.at[t, row], sem("wo", t))
        for d in (1, 3, 2):
            got(w_hbm.at[t, row], sem("wf", 3 * t + d - 1))

    w_issue(0)
    send(wout, wo_hbm, partner, sem("wout"))

    for d in range(1, ny):
        got(stat.at[d], sem("stat", d - 1))

    def norm(i, _):
        at = pl.ds(pl.multiple_of(i * 32, 32), 32)
        total = (stat[0, at, :] + stat[1, at, :]) + (stat[2, at, :] + stat[3, at, :])
        mean = total[:, 0:1] / d_model
        var = total[:, 1:2] / d_model - mean * mean
        v = xv[at, :].astype(jnp.float32)
        z[cx, cy, at, :] = ((v - mean) * lax.rsqrt(var + NORM_EPS) * gain_ref[...]).astype(z.dtype)
        return 0

    lax.fori_loop(0, tok // 32, norm, 0)

    off = (0, 1, 3, 2)
    lo, hi = pl.ds(0, half), pl.ds(half, half)

    def zb(b, dy, rows=None):
        ref = z.at[ring(cx, off[b], nx), ring(cy, dy, ny)]
        return ref if rows is None else ref.at[rows]

    def zx_send():
        send(zb(0, 0), zb(0, 0), dev(dx=1), sem("zx", 0), z_sends)
        send(zb(0, 0), zb(0, 0), dev(dx=-1), sem("zx", 1), z_sends)

    def zx_forward():
        got(zb(2, 0), sem("zx", 0))
        send(zb(2, 0, lo), zb(2, 0, lo), dev(dx=1), sem("zx", 2), z_sends)
        got(zb(1, 0), sem("zx", 1))
        send(zb(1, 0, hi), zb(1, 0, hi), dev(dx=-1), sem("zx", 3), z_sends)

    def zx_last():
        got(zb(3, 0, lo), sem("zx", 2))
        got(zb(3, 0, hi), sem("zx", 3))

    def zy_send(b):
        send(zb(b, 0), zb(b, 0), dev(dy=1), sem("zy", 4 * b), z_sends)
        send(zb(b, 0), zb(b, 0), dev(dy=-1), sem("zy", 4 * b + 1), z_sends)

    def zy_forward(b):
        got(zb(b, -1), sem("zy", 4 * b))
        send(zb(b, -1, lo), zb(b, -1, lo), dev(dy=1), sem("zy", 4 * b + 2), z_sends)
        got(zb(b, 1), sem("zy", 4 * b + 1))
        send(zb(b, 1, hi), zb(b, 1, hi), dev(dy=-1), sem("zy", 4 * b + 3), z_sends)

    def zy_last(b):
        got(zb(b, 2, lo), sem("zy", 4 * b + 2))
        got(zb(b, 2, hi), sem("zy", 4 * b + 3))

    def wt_load(t, slot):
        for j in range(2 * nx):
            r = ring(row, j, 2 * nx)
            dst = wt.at[slot, r // 2, pl.ds(pl.multiple_of(lax.rem(r, 2) * krows, krows), krows)]
            src = win.at[:, columns(0, t)] if j == 0 else w_hbm.at[t, r]
            pltpu.make_async_copy(src, dst, ls.at[1 + slot]).start()

    def wt_wait(slot):
        pltpu.make_async_copy(wt.at[slot], wt.at[slot], ls.at[1 + slot]).wait()

    def up(hm, hf, first, t0, t1, b0, b1):
        wt_load(t0, 0)

        def tile(i, _):
            slot = lax.rem(i, 2)
            wt_wait(slot)

            @pl.when(i + 1 < t1 - t0)
            def _():
                wt_load(t0 + i + 1, 1 - slot)

            at = pl.ds(pl.multiple_of((t0 + i - first) * tw, 128), tw)

            def rows(b, _):
                t = ring(cx, b + b // 2 - 2 * (b // 3), nx)
                v = jnp.dot(z[t, 0], wt[slot, 0], preferred_element_type=jnp.float32)
                for j in range(1, ny):
                    v += jnp.dot(z[t, j], wt[slot, j], preferred_element_type=jnp.float32)
                h = gelu(v).astype(hm.dtype).reshape(SUB, sub, tw)
                hm[t, :, :, at] = h

                @pl.when((t == cy) & (cx == cy))
                def _():
                    hf[cx, :, cy, :, at] = h

                return 0

            lax.fori_loop(b0, b1, rows, 0)
            return 0

        lax.fori_loop(0, t1 - t0, tile, 0)

    def h1_a():
        for d in range(1, ny):
            t = ring(cy, d, ny)
            i = sem("h1a", d - 1)

            @pl.when(cx == cy)
            def _():
                remote(hm_a.at[t], hf_a.at[cx, :, t], dev(dy=d), i).start()

            @pl.when(cx != cy)
            def _():
                remote(hm_a.at[t], hst_a.at[cy], dev(dy=d), i).start()

            sends.append(remote(hm_a.at[t], hst_a.at[cy], dev(dy=d), i))

    def h1_b(s):
        for d in range(1, ny):
            t = ring(cy, d, ny)
            i = sem("h1b", 3 * s + d - 1)

            @pl.when(cx == cy)
            def _():
                remote(hm_b.at[t, s], hf_b.at[cx, s, t], dev(dy=d), i).start()

            @pl.when(cx != cy)
            def _():
                remote(hm_b.at[t, s], hst_b.at[cy, s], dev(dy=d), i).start()

            sends.append(remote(hm_b.at[t, s], hst_b.at[cy, s], dev(dy=d), i))

    def h1_wait(ref, first):
        for d in range(1, ny):
            got(ref, first + d - 1)

    def h2(late, s):
        hm, hst, hf = (hm_b, hst_b, hf_b) if late else (hm_a, hst_a, hf_a)
        for d in (1, 3, 2):
            c = ring(cx, d, nx)
            i = sem("h2", 3 * (late * SUB + s) + d - 1)

            @pl.when(c == cy)
            def _():
                remote(hm.at[cy, s], hf.at[cx, s, cy], dev(dx=d), i).start()

            @pl.when(c != cy)
            def _():
                remote(hst.at[c, s], hf.at[cx, s, cy], dev(dx=d), i).start()

            sends.append(remote(hst.at[c, s], hf.at[cx, s, cy], dev(dx=d), i))

    def ag(late, s):
        hf = hf_b if late else hf_a
        u = late * SUB + s
        for d in (1, 3, 2):
            got(hf.at[ring(cx, -d, nx), s, cy], sem("h2", 3 * u + d - 1))
        mine = hf.at[:, s, cy]
        send(mine, mine, dev(dy=1), sem("ag", 4 * u))
        send(mine, mine, dev(dy=-1), sem("ag", 4 * u + 1))

    def ag_forward(late, s):
        hf = hf_b if late else hf_a
        u = late * SUB + s
        left, right = ring(cy, -1, ny), ring(cy, 1, ny)
        first, second = pl.ds(0, nx // 2), pl.ds(nx // 2, nx // 2)
        got(hf.at[:, s, left], sem("ag", 4 * u))
        send(hf.at[first, s, left], hf.at[first, s, left], dev(dy=1), sem("ag", 4 * u + 2))
        got(hf.at[:, s, right], sem("ag", 4 * u + 1))
        send(hf.at[second, s, right], hf.at[second, s, right], dev(dy=-1), sem("ag", 4 * u + 3))

    def ag_last(late, s):
        hf = hf_b if late else hf_a
        u = late * SUB + s
        far = ring(cy, 2, ny)
        got(hf.at[pl.ds(0, nx // 2), s, far], sem("ag", 4 * u + 2))
        got(hf.at[pl.ds(nx // 2, nx // 2), s, far], sem("ag", 4 * u + 3))

    ew, lw = early * tw, LATE * tw
    depth = wot.shape[1]
    per = ew // depth

    def wot_load(i, slot):
        u, j = i // per, lax.rem(i, per)
        c = 2 * lax.rem(k + u // 2, 2) + lax.rem(u, 2)
        at = pl.ds(pl.multiple_of(lax.rem(u, 2) * (ew + lw) + j * depth, 128), depth)

        @pl.when(u < nx // 2)
        def _():
            pltpu.make_async_copy(wout.at[at], wot.at[slot], ls.at[3 + slot]).start()

        @pl.when(u >= nx // 2)
        def _():
            pltpu.make_async_copy(wo_hbm.at[at], wot.at[slot], ls.at[3 + slot]).start()

        return c, j

    def down_early():
        wot_load(0, 0)

        def step(i, _):
            slot = lax.rem(i, 2)
            pltpu.make_async_copy(wot.at[slot], wot.at[slot], ls.at[3 + slot]).wait()

            @pl.when(i + 1 < nx * per)
            def _():
                wot_load(i + 1, 1 - slot)

            u, j = i // per, lax.rem(i, per)
            c = 2 * lax.rem(k + u // 2, 2) + lax.rem(u, 2)
            at = pl.ds(pl.multiple_of(j * depth, 128), depth)

            def rows(s, _):
                h = hf_a[c, s, :, :, at].reshape(tok, depth)
                v = jnp.dot(h, wot[slot], preferred_element_type=jnp.float32).reshape(acc.shape[1:])

                @pl.when(i == 0)
                def _():
                    acc[s] = v

                @pl.when(i > 0)
                def _():
                    acc[s] += v

                return 0

            lax.fori_loop(0, SUB, rows, 0)
            return 0

        lax.fori_loop(0, nx * per, step, 0)

    def late_weights():
        n3 = lw // tok
        for c in z_sends:
            c.wait_send()

        def fetch(i, _):
            u, j = i // n3, lax.rem(i, n3)
            c = 2 * lax.rem(k + u // 2, 2) + lax.rem(u, 2)
            at = pl.ds(pl.multiple_of(lax.rem(u, 2) * (ew + lw) + ew + j * tok, 128), tok)

            @pl.when(u < nx // 2)
            def _():
                pltpu.make_async_copy(wout.at[at], z.at[c, j], ls.at[5]).start()

            @pl.when(u >= nx // 2)
            def _():
                pltpu.make_async_copy(wo_hbm.at[at], z.at[c, j], ls.at[5]).start()

            return 0

        lax.fori_loop(0, nx * n3, fetch, 0)
        ref = z.at[:, pl.ds(0, n3)]
        pltpu.make_async_copy(ref, ref, ls.at[5]).wait()

    def down_late(s):
        n3 = lw // tok

        def step(c, _):
            h = hf_b[c, s].reshape(tok, lw)
            w = z[c, pl.ds(0, n3)].reshape(lw, dloc)
            acc[s] += jnp.dot(h, w, preferred_element_type=jnp.float32).reshape(acc.shape[1:])
            return 0

        lax.fori_loop(0, nx, step, 0)

    def y_send(s):
        for d in (2, 1, 3):
            send(acc.at[s, ring(cx, d, nx)], yr_hbm.at[d - 1, s], dev(dx=d), sem("y", 3 * s + d - 1))

    def y_final(s):
        for d in range(1, nx):
            got(yr_hbm.at[d - 1, s], sem("y", 3 * s + d - 1))
        c = pltpu.make_async_copy(yr_hbm.at[:, s], yt, ls.at[6])
        c.start()
        c.wait()
        at = pl.ds(s * sub, sub)
        total = (acc[s, cx] + yt[0]) + (yt[1] + yt[2])
        ov[at, :] = (xv[at, :].astype(jnp.float32) + total).astype(ov.dtype)

    zy_send(0)
    zx_send()
    w_issue(1)
    zy_forward(0)
    zx_forward()
    zy_send(1)
    zy_send(2)
    w_forward(0)
    w_issue(2)
    zy_last(0)
    zx_last()
    zy_send(3)
    zy_forward(1)
    zy_forward(2)
    w_forward(1)
    w_issue(3)
    zy_last(1)
    zy_last(2)
    w_forward(2)
    w_issue(4)
    zy_forward(3)
    w_ready(0)
    w_ready(1)
    w_ready(2)
    up(hm_a, hf_a, 0, 0, 3, 0, 3)
    w_forward(3)
    w_issue(5)
    w_ready(3)
    up(hm_a, hf_a, 0, 3, 4, 0, 3)
    zy_last(3)
    up(hm_a, hf_a, 0, 0, 4, 3, 4)
    h1_a()
    w_forward(4)
    w_issue(6)
    h1_wait(hst_a.at[0], sem("h1a"))
    for s in range(SUB):
        h2(0, s)
    w_ready(4)
    up(hm_b, hf_b, early, 4, 5, 0, 4)
    for s in range(SUB):
        ag(0, s)
    w_forward(5)
    w_ready(5)
    up(hm_b, hf_b, early, 5, 6, 0, 4)
    w_forward(6)
    for s in range(SUB):
        ag_forward(0, s)
    w_ready(6)
    up(hm_b, hf_b, early, 6, 7, 0, 4)
    for s in range(SUB):
        h1_b(s)
    for s in range(SUB):
        ag_last(0, s)
    got(wo_hbm, sem("wout"))
    down_early()
    late_weights()
    for s in range(SUB):
        h1_wait(hst_b.at[0, 0], sem("h1b", 3 * s))
        h2(1, s)
    for s in range(SUB):
        ag(1, s)
    for s in range(SUB):
        ag_forward(1, s)
    for s in range(SUB):
        ag_last(1, s)
        down_late(s)
        y_send(s)
        if s > 0:
            y_final(s - 1)
    y_final(SUB - 1)
    out = pltpu.make_async_copy(ov, y_hbm, ls.at[0])
    out.start()
    for c in sends:
        c.wait_send()
    out.wait()


def solution(mesh):
    nx, ny = mesh.shape["row"] // 2, mesh.shape["col"]

    def local_block(x, gain, win, wout):
        tok, dloc = x.shape
        krows, floc = win.shape
        width = floc // nx
        tw = width // 7
        tiles = width // tw
        early = tiles - LATE
        ew, lw = early * tw, LATE * tw
        sub = tok // SUB
        bf, f32 = jnp.bfloat16, jnp.float32
        count = plan(tiles).total
        hbm = lambda shape, dt: jax.ShapeDtypeStruct(shape, dt)
        outs = pl.pallas_call(
            functools.partial(block, (nx, ny, dloc * ny)),
            name="mlp_block",
            out_shape=[
                hbm((tok, dloc), bf),
                hbm((tiles, 2 * nx, krows, tw), bf),
                hbm(wout.shape, bf),
                hbm((ny, SUB, sub, ew), bf),
                hbm((ny, SUB, sub, lw), bf),
                hbm((nx - 1, SUB, sub, dloc), f32),
            ],
            in_specs=[
                pl.BlockSpec(memory_space=pl.ANY),
                pl.BlockSpec(memory_space=pltpu.VMEM),
                pl.BlockSpec(memory_space=pl.ANY),
                pl.BlockSpec(memory_space=pl.ANY),
            ],
            out_specs=[pl.BlockSpec(memory_space=pl.ANY)] * 6,
            scratch_shapes=[
                pltpu.VMEM((tok, dloc), bf),
                pltpu.VMEM((ny, tok, 128), f32),
                pltpu.VMEM((nx, ny, tok, dloc), bf),
                pltpu.VMEM((2, ny, 2 * krows, tw), bf),
                pltpu.VMEM((nx, SUB, sub, ew), bf),
                pltpu.VMEM((nx, SUB, sub, lw), bf),
                pltpu.VMEM((nx, SUB, ny, sub, ew), bf),
                pltpu.VMEM((nx, SUB, ny, sub, lw), bf),
                pltpu.VMEM((SUB, nx, sub, dloc), f32),
                pltpu.VMEM((2, 2 * tw, dloc), bf),
                pltpu.VMEM((nx - 1, sub, dloc), f32),
                pltpu.VMEM((tok, dloc), bf),
                pltpu.SemaphoreType.DMA((count,)),
                pltpu.SemaphoreType.DMA((count,)),
                pltpu.SemaphoreType.DMA((7,)),
            ],
            compiler_params=pltpu.CompilerParams(
                collective_id=0, has_side_effects=True, vmem_limit_bytes=67043328
            ),
        )(x, gain.reshape(1, dloc), win, wout)
        return outs[0]

    return jax.shard_map(
        local_block,
        mesh=mesh,
        in_specs=(P(("dp", "row"), "col"), P("col"), P("row", "col"), P("row", "col")),
        out_specs=P(("dp", "row"), "col"),
        check_vma=False,
    )
```

```python
import functools

import jax
import jax.numpy as jnp
from jax import lax
from jax.experimental import pallas as pl
from jax.experimental.pallas import tpu as pltpu
from jax.sharding import PartitionSpec as P

NORM_EPS = 1e-5
MESH = pl.DeviceIdType.MESH
SUB = 4
LATE = 3


def gelu(v):
    return 0.5 * v * (1.0 + jnp.tanh(0.7978845608028654 * (v + 0.044715 * (v * v * v))))


class Sems:
    def __init__(self):
        self.base, self.total = {}, 0

    def add(self, name, count):
        self.base[name] = self.total
        self.total += count

    def __call__(self, name, index=0):
        return self.base[name] + index


def plan(tiles):
    s = Sems()
    for name, count in (
        ("stat", 3), ("gain", 3), ("mean", 2), ("zx", 4), ("zy", 16), ("w", 3 * tiles), ("wo", tiles), ("wf", 3 * tiles),
        ("wout", 1), ("h1a", 12), ("h1b", 3 * SUB), ("h2a", 12), ("h2b", 3 * SUB), ("aga", 16), ("agb", 4 * SUB), ("y", 6 * SUB),
    ):
        s.add(name, count)
    return s


def block(n, x_hbm, gain_ref, win, wout, y_hbm, w_hbm, wo_hbm, hst_a, hst_b,
          xv, sums, stat, means, gains, z, wt, hm_a, hm_b, hf_a, hf_b, acc, ya, yb, ov, ss, rs, ls):
    nx, ny, d_model = n
    row, cy = lax.axis_index("row"), lax.axis_index("col")
    cx, k = row // 2, lax.rem(row, 2)
    tok, dloc = ov.shape
    tiles, krows, tw = w_hbm.shape[0], w_hbm.shape[2], w_hbm.shape[3]
    early = tiles - LATE
    half = tok // 2
    sub = tok // SUB
    piece = sub // ny
    sem = plan(tiles)

    def ring(v, d, m):
        return lax.rem(v + (d + m), m)

    def dev(dx=0, dy=0, core=None):
        return {"row": 2 * ring(cx, dx, nx) + (k if core is None else core), "col": ring(cy, dy, ny)}

    partner = dev(core=1 - k)

    def remote(src, dst, where, i):
        return pltpu.make_async_remote_copy(
            src_ref=src, dst_ref=dst, send_sem=ss.at[i], recv_sem=rs.at[i], device_id=where, device_id_type=MESH
        )

    sends, z_sends = [], []

    def send(src, dst, where, i, log=sends):
        c = remote(src, dst, where, i)
        c.start()
        log.append(c)

    def got(ref, i):
        remote(ref, ref, partner, i).wait_recv()

    load_x = pltpu.make_async_copy(x_hbm, xv, ls.at[0])
    load_x.start()
    barrier = pltpu.get_barrier_semaphore()
    peers = [partner] + [dev(dx=d) for d in range(1, nx)] + [dev(dy=d) for d in range(1, ny)]
    for p in peers:
        pl.semaphore_signal(barrier, inc=1, device_id=p, device_id_type=MESH)
    load_x.wait()

    lane = lax.broadcasted_iota(jnp.int32, (32, sums.shape[2]), 1)

    def part(i, _):
        at = pl.ds(pl.multiple_of(i * 32, 32), 32)
        v = xv[at, :].astype(jnp.float32)
        s1 = jnp.sum(v, axis=1, keepdims=True)
        s2 = jnp.sum(v * v, axis=1, keepdims=True)
        sums[0, at, :] = jnp.where(lane == 0, s1, s2)
        return 0

    lax.fori_loop(0, tok // 32, part, 0)
    stat[cy] = jnp.transpose(sums[0])[: stat.shape[1]]
    gains[cy] = gain_ref[...]
    pl.semaphore_wait(barrier, len(peers))
    for d in (1, 3, 2):
        send(stat.at[cy], stat.at[cy], dev(dy=d), sem("stat", d - 1))
    for d in (1, 3, 2):
        send(gains.at[cy], gains.at[cy], dev(dy=d), sem("gain", d - 1))

    off = (0, 1, 3, 2)
    lo, hi = pl.ds(0, half), pl.ds(half, half)

    def zb(b, dy, rows=None):
        ref = z.at[ring(cx, off[b], nx), ring(cy, dy, ny)]
        return ref if rows is None else ref.at[rows]

    for d in (1, -1):
        send(xv, zb(0, 0), dev(dy=d), sem("zy", 0 if d == 1 else 1))
    for d in (1, -1):
        send(xv, zb(0, 0), dev(dx=d), sem("zx", 0 if d == 1 else 1))

    def columns(dx, t):
        return pl.ds(pl.multiple_of(ring(cx, dx, nx) * (tiles * tw) + t * tw, 128), tw)

    def w_issue(t):
        for d in (1, 3, 2):
            send(win.at[:, columns(d, t)], w_hbm.at[t, row], dev(dx=d), sem("w", 3 * t + d - 1))
        send(win.at[:, columns(0, t)], w_hbm.at[t, row], partner, sem("wo", t))

    def w_forward(t):
        for d in (1, 3, 2):
            slot = 2 * ring(cx, -d, nx) + k
            got(w_hbm.at[t, slot], sem("w", 3 * t + d - 1))
            send(w_hbm.at[t, slot], w_hbm.at[t, slot], partner, sem("wf", 3 * t + d - 1))

    def w_ready(t):
        got(w_hbm.at[t, row], sem("wo", t))
        for d in (1, 3, 2):
            got(w_hbm.at[t, row], sem("wf", 3 * t + d - 1))

    for d in range(1, ny):
        got(stat.at[0], sem("stat", d - 1))
    total = (stat[0] + stat[1]) + (stat[2] + stat[3])
    mean = total[0:1] / d_model
    rstd = lax.rsqrt(total[1:2] / d_model - mean * mean + NORM_EPS)
    means[0] = jnp.where(lax.broadcasted_iota(jnp.int32, total.shape, 0) == 0, mean, rstd)
    send(means.at[0], means.at[2], dev(dx=1), sem("mean", 0))
    send(means.at[0], means.at[1], dev(dx=-1), sem("mean", 1))
    w_issue(0)
    send(wout, wo_hbm, partner, sem("wout"))

    def spread(b):
        copies = sums.shape[2] // means.shape[1]
        sums[b] = jnp.transpose(jnp.concatenate([means[b]] * copies, axis=0))

    def normalise(b, y, src=None):
        t = ring(cx, off[b], nx)

        def norm(i, _):
            at = pl.ds(pl.multiple_of(i * 32, 32), 32)
            v = (z[t, y, at, :] if src is None else src[at, :]).astype(jnp.float32)
            z[t, y, at, :] = ((v - sums[b, at, 0:1]) * sums[b, at, 1:2] * gains[y]).astype(z.dtype)
            return 0

        lax.fori_loop(0, tok // 32, norm, 0)

    spread(0)
    normalise(0, cy, xv)

    up_y, down_y, far_y = ring(cy, 1, ny), ring(cy, -1, ny), ring(cy, 2, ny)

    def zx_forward():
        got(xv, sem("zx", 0))
        got(means.at[0], sem("mean", 0))
        spread(2)
        normalise(2, cy)
        send(zb(2, 0, lo), zb(2, 0, lo), dev(dx=1), sem("zx", 2), z_sends)
        zy_send(2)
        got(xv, sem("zx", 1))
        got(means.at[0], sem("mean", 1))
        spread(1)
        normalise(1, cy)
        send(zb(1, 0, hi), zb(1, 0, hi), dev(dx=-1), sem("zx", 3), z_sends)
        zy_send(1)

    def zx_last():
        got(zb(3, 0, lo), sem("zx", 2))
        got(zb(3, 0, hi), sem("zx", 3))

    def zy_send(b):
        send(zb(b, 0), zb(b, 0), dev(dy=1), sem("zy", 4 * b), z_sends)
        send(zb(b, 0), zb(b, 0), dev(dy=-1), sem("zy", 4 * b + 1), z_sends)

    def zy_forward(b):
        got(zb(b, -1), sem("zy", 4 * b))
        send(zb(b, -1, lo), zb(b, -1, lo), dev(dy=1), sem("zy", 4 * b + 2), z_sends)
        got(zb(b, 1), sem("zy", 4 * b + 1))
        send(zb(b, 1, hi), zb(b, 1, hi), dev(dy=-1), sem("zy", 4 * b + 3), z_sends)

    def zy_last(b):
        got(zb(b, 2, lo), sem("zy", 4 * b + 2))
        got(zb(b, 2, hi), sem("zy", 4 * b + 3))

    def zy_forward_own():
        got(xv, sem("zy", 0))
        for d in range(1, ny):
            got(gains.at[0], sem("gain", d - 1))
        normalise(0, down_y)
        send(zb(0, -1, lo), zb(0, -1, lo), dev(dy=1), sem("zy", 2), z_sends)
        got(xv, sem("zy", 1))
        normalise(0, up_y)
        send(zb(0, 1, hi), zb(0, 1, hi), dev(dy=-1), sem("zy", 3), z_sends)

    def wt_load(t, slot):
        for j in range(2 * nx):
            r = ring(row, j, 2 * nx)
            dst = wt.at[slot, r // 2, pl.ds(pl.multiple_of(lax.rem(r, 2) * krows, krows), krows)]
            src = win.at[:, columns(0, t)] if j == 0 else w_hbm.at[t, r]
            pltpu.make_async_copy(src, dst, ls.at[1 + slot]).start()

    def wt_wait(slot):
        pltpu.make_async_copy(wt.at[slot], wt.at[slot], ls.at[1 + slot]).wait()

    def up_load(t0, t1):
        for i in range(min(2, t1 - t0)):
            wt_load(t0 + i, i)

    def up(late, t0, t1, b0, b1, loaded=False):
        hm, hf, first = (hm_b, hf_b, early) if late else (hm_a, hf_a, 0)
        if not loaded:
            up_load(t0, t1)

        def tile(i, _):
            slot = lax.rem(i, 3)
            wt_wait(slot)

            @pl.when(i + 2 < t1 - t0)
            def _():
                wt_load(t0 + i + 2, lax.rem(i + 2, 3))

            at = pl.ds(pl.multiple_of((t0 + i - first) * tw, 128), tw)

            def rows(b, _):
                t = ring(cx, b + b // 2 - 2 * (b // 3), nx)
                v = jnp.dot(z[t, 0], wt[slot, 0], preferred_element_type=jnp.float32)
                for j in range(1, ny):
                    v += jnp.dot(z[t, j], wt[slot, j], preferred_element_type=jnp.float32)
                hm[t, :, :, :, at] = gelu(v).astype(hm.dtype).reshape(ny, SUB, piece, tw)

                @pl.when(cx == cy)
                def _():
                    hf[cx, :, t, cy, :, at] = hm[t, cy, :, :, at]

                return 0

            lax.fori_loop(b0, b1, rows, 0)
            return 0

        lax.fori_loop(0, t1 - t0, tile, 0)

    def h1_a(b):
        t = ring(cx, off[b], nx)
        for d in (1, 3, 2):
            c = ring(cy, d, ny)
            i = sem("h1a", 3 * b + d - 1)

            @pl.when(cx == cy)
            def _():
                remote(hm_a.at[t, c], hf_a.at[cx, :, t, c], dev(dy=d), i).start()

            @pl.when(cx != cy)
            def _():
                remote(hm_a.at[t, c], hst_a.at[cy, :, t], dev(dy=d), i).start()

            sends.append(remote(hm_a.at[t, c], hst_a.at[cy, :, t], dev(dy=d), i))

    def h2_a(b):
        t = ring(cx, off[b], nx)
        for d in range(1, ny):
            got(hst_a.at[0, :, 0], sem("h1a", 3 * b + d - 1))
        for d in (1, 3, 2):
            c = ring(cx, d, nx)
            i = sem("h2a", 3 * b + d - 1)

            @pl.when(c == cy)
            def _():
                remote(hm_a.at[t, cy], hf_a.at[cx, :, t, cy], dev(dx=d), i).start()

            @pl.when(c != cy)
            def _():
                remote(hst_a.at[c, :, t], hf_a.at[cx, :, t, cy], dev(dx=d), i).start()

            sends.append(remote(hst_a.at[c, :, t], hf_a.at[cx, :, t, cy], dev(dx=d), i))

    def h1_b(s):
        for d in (1, 3, 2):
            c = ring(cy, d, ny)
            i = sem("h1b", 3 * s + d - 1)

            @pl.when(cx == cy)
            def _():
                remote(hm_b.at[:, c, s], hf_b.at[cx, s, :, c], dev(dy=d), i).start()

            @pl.when(cx != cy)
            def _():
                remote(hm_b.at[:, c, s], hst_b.at[cy, s], dev(dy=d), i).start()

            sends.append(remote(hm_b.at[:, c, s], hst_b.at[cy, s], dev(dy=d), i))

    def h2_b(s):
        for d in range(1, ny):
            got(hst_b.at[0, 0], sem("h1b", 3 * s + d - 1))
        for d in (1, 3, 2):
            c = ring(cx, d, nx)
            i = sem("h2b", 3 * s + d - 1)

            @pl.when(c == cy)
            def _():
                remote(hm_b.at[:, cy, s], hf_b.at[cx, s, :, cy], dev(dx=d), i).start()

            @pl.when(c != cy)
            def _():
                remote(hst_b.at[c, s], hf_b.at[cx, s, :, cy], dev(dx=d), i).start()

            sends.append(remote(hst_b.at[c, s], hf_b.at[cx, s, :, cy], dev(dx=d), i))

    x_low, x_high = pl.ds(0, nx // 2), pl.ds(nx // 2, nx // 2)

    def gather(name, index, part):
        everything = pl.ds(0, nx)
        i = sem(name, 4 * index)

        def begin():
            send(part(everything, cy), part(everything, cy), dev(dy=1), i)
            send(part(everything, cy), part(everything, cy), dev(dy=-1), i + 1)

        def forward():
            got(part(everything, cy), i)
            send(part(x_low, down_y), part(x_low, down_y), dev(dy=1), i + 2)
            got(part(everything, cy), i + 1)
            send(part(x_high, up_y), part(x_high, up_y), dev(dy=-1), i + 3)

        def last():
            got(part(x_low, far_y), i + 2)
            got(part(x_high, far_y), i + 3)

        return begin, forward, last

    gather_a = [gather("aga", b, lambda c, y, b=b: hf_a.at[c, :, ring(cx, off[b], nx), y]) for b in range(nx)]
    gather_b = [gather("agb", s, lambda c, y, s=s: hf_b.at[c, s, :, y]) for s in range(SUB)]

    def ag_a(b):
        for d in range(1, nx):
            got(hst_a.at[0, :, 0], sem("h2a", 3 * off.index((off[b] + d) % nx) + d - 1))
        gather_a[b][0]()

    def ag_a_forward(b):
        gather_a[b][1]()

    def ag_a_last(b):
        gather_a[b][2]()

    def ag_b(s):
        for d in range(1, nx):
            got(hst_b.at[0, 0], sem("h2b", 3 * s + d - 1))
        gather_b[s][0]()

    def ag_b_forward(s):
        gather_b[s][1]()

    def ag_b_last(s):
        gather_b[s][2]()

    ew, lw = early * tw, LATE * tw
    npt = 2 * krows // ew
    steps = dloc // (npt * tw)
    kept = lw // tok

    def rows_of(c, skip, count, use):
        at = pl.ds(pl.multiple_of(lax.rem(c, 2) * (ew + lw) + skip, 128), count)

        @pl.when(c // 2 == k)
        def _():
            use(wout, at)

        @pl.when(c // 2 != k)
        def _():
            use(wo_hbm, at)

    def we_load(i, slot):
        for c in range(nx):
            for j in range(npt):
                cols = pl.ds(pl.multiple_of((i * npt + j) * tw, 128), tw)
                dst = wt.at[slot, c, pl.ds(j * ew, ew)]
                rows_of(c, 0, ew, lambda ref, at: pltpu.make_async_copy(ref.at[at, cols], dst, ls.at[1 + slot]).start())

    def we_wait(slot):
        ref = wt.at[slot, :, pl.ds(0, npt * ew)]
        pltpu.make_async_copy(ref, ref, ls.at[1 + slot]).wait()

    def down_early_load():
        for i in range(min(2, steps)):
            we_load(i, i)

    def down_early(b0, b1, loaded=False):
        if not loaded:
            down_early_load()

        def step(i, _):
            slot = lax.rem(i, 3)
            we_wait(slot)

            @pl.when(i + 2 < steps)
            def _():
                we_load(i + 2, lax.rem(i + 2, 3))

            def rows(b, _):
                t = ring(cx, b + b // 2 - 2 * (b // 3), nx)
                for j in range(npt):
                    v = None
                    for c in range(nx):
                        h = hf_a[c, :, t].reshape(tok, ew)
                        p = jnp.dot(h, wt[slot, c, pl.ds(j * ew, ew)], preferred_element_type=jnp.float32)
                        v = p if v is None else v + p
                    cols = pl.ds(pl.multiple_of((i * npt + j) * tw, 128), tw)
                    acc[:, t, :, cols] = v.reshape(SUB, sub, tw)
                return 0

            lax.fori_loop(b0, b1, rows, 0)
            return 0

        lax.fori_loop(0, steps, step, 0)

    def late_start():
        for c in z_sends:
            c.wait_send()
        for c in range(nx):
            for j in range(kept):
                rows_of(c, ew + j * tok, tok, lambda ref, at: pltpu.make_async_copy(ref.at[at], z.at[c, j], ls.at[4]).start())

    def late_wait():
        ref = z.at[:, pl.ds(0, kept)]
        pltpu.make_async_copy(ref, ref, ls.at[4]).wait()

    def down_late(s):
        wide = 2 * tw

        def step(i, _):
            cols = pl.ds(pl.multiple_of(i * wide, 128), wide)
            v = None
            for c in range(nx):
                h = hf_b[c, s].reshape(nx * sub, lw)
                p = jnp.dot(h, z[c, pl.ds(0, kept), :, cols].reshape(lw, wide), preferred_element_type=jnp.float32)
                v = p if v is None else v + p
            acc[s, :, :, cols] += v.reshape(nx, sub, wide)
            return 0

        lax.fori_loop(0, dloc // wide, step, 0)

    top, low = pl.ds(0, sub // 2), pl.ds(sub // 2, sub // 2)
    right, left, across = ring(cx, 1, nx), ring(cx, -1, nx), ring(cx, 2, nx)

    def y_send(s):
        send(acc.at[s, across, top], ya.at[s, 0], dev(dx=1), sem("y", 6 * s))
        send(acc.at[s, across, low], ya.at[s, 1], dev(dx=-1), sem("y", 6 * s + 1))
        send(acc.at[s, right, low], yb.at[s, 0, low], dev(dx=1), sem("y", 6 * s + 2))
        send(acc.at[s, left, top], yb.at[s, 1, top], dev(dx=-1), sem("y", 6 * s + 3))

    def y_forward(s):
        got(ya.at[s, 0], sem("y", 6 * s))
        acc[s, right, top] += ya[s, 0]
        send(acc.at[s, right, top], yb.at[s, 0, top], dev(dx=1), sem("y", 6 * s + 4))
        got(ya.at[s, 1], sem("y", 6 * s + 1))
        acc[s, left, low] += ya[s, 1]
        send(acc.at[s, left, low], yb.at[s, 1, low], dev(dx=-1), sem("y", 6 * s + 5))

    def y_final(s):
        for j in range(2, 6):
            got(ya.at[s, 0], sem("y", 6 * s + j))
        for c in range(ny):
            rows, at = pl.ds(c * piece, piece), pl.ds(c * sub + s * piece, piece)
            total = acc[s, cx, rows] + (yb[s, 0, rows] + yb[s, 1, rows])
            ov[at, :] = (xv[at, :].astype(jnp.float32) + total).astype(ov.dtype)

    n0, n1, n2, n3, n4, n5, n6, n7 = range(8)
    zy_forward_own()
    zx_forward()
    w_issue(n1)
    w_issue(n2)
    w_issue(n3)
    w_issue(n4)
    w_forward(n0)
    zy_forward(n2)
    zx_last()
    zy_send(n3)
    w_forward(n1)
    w_forward(n2)
    zy_last(n0)
    w_ready(n1)
    up(n0, n1, n2, n0, n1)
    w_ready(n0)
    up(n0, n0, n1, n0, n1)
    zy_last(n2)
    w_ready(n2)
    up(n0, n2, n3, n0, n1)
    zy_forward(n1)
    up(n0, n0, n3, n2, n3)
    w_forward(n3)
    zy_forward(n3)
    zy_last(n1)
    w_ready(n3)
    up(n0, n3, n4, n0, n3)
    h1_a(n2)
    h1_a(n0)
    zy_last(n3)
    up(n0, n0, n4, n3, n4)
    h2_a(n2)
    h1_a(n3)
    h2_a(n0)
    up(n0, n0, n3, n1, n2)
    h1_a(n1)
    h2_a(n3)
    h2_a(n1)
    ag_a(n1)
    w_issue(n5)
    ag_a(n0)
    w_forward(n4)
    w_ready(n4)
    up(n1, n4, n5, n0, n4)
    w_issue(n6)
    ag_a(n3)
    ag_a_forward(n1)
    w_forward(n5)
    ag_a_forward(n3)
    w_ready(n5)
    up(n1, n5, n6, n0, n4)
    ag_a(n2)
    w_forward(n6)
    ag_a_last(n3)
    ag_a_forward(n0)
    got(wo_hbm, sem("wout"))
    down_early(n3, n4)
    ag_a_forward(n2)
    w_ready(n6)
    up(n1, n6, n7, n0, n4)
    h1_b(n0)
    h1_b(n1)
    ag_a_last(n0)
    down_early(n0, n1)
    h2_b(n0)
    ag_a_last(n1)
    ag_a_last(n2)
    h1_b(n2)
    late_start()
    h2_b(n1)
    ag_b(n0)
    down_early(n2, n3)
    h1_b(n3)
    h2_b(n2)
    ag_b_forward(n0)
    down_early(n1, n2)
    late_wait()
    h2_b(n3)
    ag_b(n1)
    ag_b_last(n0)
    down_late(n0)
    y_send(n0)
    ag_b_forward(n1)
    y_forward(n0)
    ag_b(n2)
    ag_b_last(n1)
    down_late(n1)
    y_send(n1)
    ag_b_forward(n2)
    y_forward(n1)
    ag_b_last(n2)
    ag_b(n3)
    down_late(n2)
    y_send(n2)
    y_final(n0)
    ag_b_forward(n3)
    y_forward(n2)
    ag_b_last(n3)
    down_late(n3)
    y_send(n3)
    y_final(n1)
    y_final(n2)
    y_forward(n3)
    y_final(n3)
    out = pltpu.make_async_copy(ov, y_hbm, ls.at[0])
    out.start()
    for c in sends:
        c.wait_send()
    out.wait()


def solution(mesh):
    nx, ny = mesh.shape["row"] // 2, mesh.shape["col"]

    def local_block(x, gain, win, wout):
        tok, dloc = x.shape
        krows, floc = win.shape
        width = floc // nx
        tw = width // 7
        tiles = width // tw
        early = tiles - LATE
        ew, lw = early * tw, LATE * tw
        sub = tok // SUB
        piece = sub // ny
        bf, f32 = jnp.bfloat16, jnp.float32
        count = plan(tiles).total
        hbm = lambda shape, dt: jax.ShapeDtypeStruct(shape, dt)
        outs = pl.pallas_call(
            functools.partial(block, (nx, ny, dloc * ny)),
            name="mlp_block",
            out_shape=[
                hbm((tok, dloc), bf),
                hbm((tiles, 2 * nx, krows, tw), bf),
                hbm(wout.shape, bf),
                hbm((ny, SUB, nx, piece, ew), bf),
                hbm((ny, SUB, nx, piece, lw), bf),
            ],
            in_specs=[
                pl.BlockSpec(memory_space=pl.ANY),
                pl.BlockSpec(memory_space=pltpu.VMEM),
                pl.BlockSpec(memory_space=pl.ANY),
                pl.BlockSpec(memory_space=pl.ANY),
            ],
            out_specs=[pl.BlockSpec(memory_space=pl.ANY)] * 5,
            scratch_shapes=[
                pltpu.VMEM((tok, dloc), bf),
                pltpu.VMEM((3, tok, 128), f32),
                pltpu.VMEM((ny, 8, tok), f32),
                pltpu.VMEM((3, 8, tok), f32),
                pltpu.VMEM((ny, 1, dloc), f32),
                pltpu.VMEM((nx, ny, tok, dloc), bf),
                pltpu.VMEM((3, ny, 2 * krows, tw), bf),
                pltpu.VMEM((nx, ny, SUB, piece, ew), bf),
                pltpu.VMEM((nx, ny, SUB, piece, lw), bf),
                pltpu.VMEM((nx, SUB, nx, ny, piece, ew), bf),
                pltpu.VMEM((nx, SUB, nx, ny, piece, lw), bf),
                pltpu.VMEM((SUB, nx, sub, dloc), f32),
                pltpu.VMEM((SUB, 2, sub // 2, dloc), f32),
                pltpu.VMEM((SUB, 2, sub, dloc), f32),
                pltpu.VMEM((tok, dloc), bf),
                pltpu.SemaphoreType.DMA((count,)),
                pltpu.SemaphoreType.DMA((count,)),
                pltpu.SemaphoreType.DMA((5,)),
            ],
            compiler_params=pltpu.CompilerParams(
                collective_id=0, has_side_effects=True, vmem_limit_bytes=67043328
            ),
        )(x, gain.reshape(1, dloc), win, wout)
        return outs[0]

    return jax.shard_map(
        local_block,
        mesh=mesh,
        in_specs=(P(("dp", "row"), "col"), P("col"), P("row", "col"), P("row", "col")),
        out_specs=P(("dp", "row"), "col"),
        check_vma=False,
    )
```

```python
import functools

import jax
import jax.numpy as jnp
from jax import lax
from jax.experimental import pallas as pl
from jax.experimental.pallas import tpu as pltpu
from jax.sharding import PartitionSpec as P

NORM_EPS = 1e-5
MESH = pl.DeviceIdType.MESH
SUB = 8
GROUPS = 4
LATE = 3


def gelu(v):
    return 0.5 * v * (1.0 + jnp.tanh(0.7978845608028654 * (v + 0.044715 * (v * v * v))))


class Sems:
    def __init__(self):
        self.base, self.total = {}, 0

    def add(self, name, count):
        self.base[name] = self.total
        self.total += count

    def __call__(self, name, index=0):
        return self.base[name] + index


def plan(tiles):
    s = Sems()
    for name, count in (
        ("stat", 3), ("gain", 3), ("mean", 2), ("zx", 4), ("zy", 16), ("w", 3 * tiles), ("wo", tiles), ("wf", 3 * tiles),
        ("wout", 1), ("h1a", 12), ("h1b", 3 * SUB), ("h2a", 12 * GROUPS), ("h2b", 3 * SUB),
        ("own", 16), ("aga", 4 * GROUPS), ("agb", 4 * SUB), ("y", 6 * SUB),
    ):
        s.add(name, count)
    return s


def block(n, x_hbm, gain_ref, win, wout, y_hbm, w_hbm, wo_hbm, hst_a, hst_b,
          xv, sums, stat, means, gains, z, wt, hm_a, hm_b, hf_a, hf_b, acc, pre, ya, yb, ov, ss, rs, ls):
    nx, ny, d_model = n
    row, cy = lax.axis_index("row"), lax.axis_index("col")
    cx, k = row // 2, lax.rem(row, 2)
    tok, dloc = ov.shape
    tiles, krows, tw = w_hbm.shape[0], w_hbm.shape[2], w_hbm.shape[3]
    early = tiles - LATE
    half = tok // 2
    sub = tok // SUB
    piece = sub // ny
    batch = SUB // GROUPS
    sem = plan(tiles)

    def ring(v, d, m):
        return lax.rem(v + (d + m), m)

    def dev(dx=0, dy=0, core=None):
        return {"row": 2 * ring(cx, dx, nx) + (k if core is None else core), "col": ring(cy, dy, ny)}

    partner = dev(core=1 - k)

    def remote(src, dst, where, i):
        return pltpu.make_async_remote_copy(
            src_ref=src, dst_ref=dst, send_sem=ss.at[i], recv_sem=rs.at[i], device_id=where, device_id_type=MESH
        )

    sends, z_sends = [], []

    def send(src, dst, where, i, log=sends):
        c = remote(src, dst, where, i)
        c.start()
        log.append(c)

    def got(ref, i):
        remote(ref, ref, partner, i).wait_recv()

    load_x = pltpu.make_async_copy(x_hbm, xv, ls.at[0])
    load_x.start()
    barrier = pltpu.get_barrier_semaphore()
    peers = [partner] + [dev(dx=d) for d in range(1, nx)] + [dev(dy=d) for d in range(1, ny)]
    for p in peers:
        pl.semaphore_signal(barrier, inc=1, device_id=p, device_id_type=MESH)
    load_x.wait()

    lane = lax.broadcasted_iota(jnp.int32, (32, sums.shape[2]), 1)

    def part(i, _):
        at = pl.ds(pl.multiple_of(i * 32, 32), 32)
        v = xv[at, :].astype(jnp.float32)
        s1 = jnp.sum(v, axis=1, keepdims=True)
        s2 = jnp.sum(v * v, axis=1, keepdims=True)
        sums[0, at, :] = jnp.where(lane == 0, s1, s2)
        return 0

    lax.fori_loop(0, tok // 32, part, 0)
    stat[cy] = jnp.transpose(sums[0])[: stat.shape[1]]
    gains[cy] = gain_ref[...]
    pl.semaphore_wait(barrier, len(peers))
    for d in (1, 3, 2):
        send(stat.at[cy], stat.at[cy], dev(dy=d), sem("stat", d - 1))
    for d in (1, 3, 2):
        send(gains.at[cy], gains.at[cy], dev(dy=d), sem("gain", d - 1))

    off = (0, 1, 3, 2)
    lo, hi = pl.ds(0, half), pl.ds(half, half)

    def zb(b, dy, rows=None):
        ref = z.at[ring(cx, off[b], nx), ring(cy, dy, ny)]
        return ref if rows is None else ref.at[rows]

    for d in (1, -1):
        send(xv, zb(0, 0), dev(dy=d), sem("zy", 0 if d == 1 else 1))
    for d in (1, -1):
        send(xv, zb(0, 0), dev(dx=d), sem("zx", 0 if d == 1 else 1))

    def columns(dx, t):
        return pl.ds(pl.multiple_of(ring(cx, dx, nx) * (tiles * tw) + t * tw, 128), tw)

    def w_issue(t):
        for d in (1, 3, 2):
            send(win.at[:, columns(d, t)], w_hbm.at[t, row], dev(dx=d), sem("w", 3 * t + d - 1))
        send(win.at[:, columns(0, t)], w_hbm.at[t, row], partner, sem("wo", t))

    def w_pass(t, ds):
        for d in ds:
            slot = 2 * ring(cx, -d, nx) + k
            got(w_hbm.at[t, slot], sem("w", 3 * t + d - 1))
            send(w_hbm.at[t, slot], w_hbm.at[t, slot], partner, sem("wf", 3 * t + d - 1))

    def w_got(t, ds):
        for d in ds:
            got(w_hbm.at[t, row], sem("wf", 3 * t + d - 1))

    def w_forward(t):
        w_pass(t, (1, 3, 2))

    def w_ready(t):
        got(w_hbm.at[t, row], sem("wo", t))
        w_got(t, (1, 3, 2))

    def w_forward_near(t):
        w_pass(t, (1, 3))

    def w_forward_far(t):
        w_pass(t, (2,))

    for d in range(1, ny):
        got(stat.at[0], sem("stat", d - 1))
    total = (stat[0] + stat[1]) + (stat[2] + stat[3])
    mean = total[0:1] / d_model
    rstd = lax.rsqrt(total[1:2] / d_model - mean * mean + NORM_EPS)
    means[0] = jnp.where(lax.broadcasted_iota(jnp.int32, total.shape, 0) == 0, mean, rstd)
    send(means.at[0], means.at[2], dev(dx=1), sem("mean", 0))
    send(means.at[0], means.at[1], dev(dx=-1), sem("mean", 1))
    w_issue(0)
    send(wout, wo_hbm, partner, sem("wout"))

    def spread(b):
        copies = sums.shape[2] // means.shape[1]
        sums[b] = jnp.transpose(jnp.concatenate([means[b]] * copies, axis=0))

    def normalise(b, y, src=None):
        t = ring(cx, off[b], nx)

        def norm(i, _):
            at = pl.ds(pl.multiple_of(i * 32, 32), 32)
            v = (z[t, y, at, :] if src is None else src[at, :]).astype(jnp.float32)
            z[t, y, at, :] = ((v - sums[b, at, 0:1]) * sums[b, at, 1:2] * gains[y]).astype(z.dtype)
            return 0

        lax.fori_loop(0, tok // 32, norm, 0)

    spread(0)
    normalise(0, cy, xv)

    up_y, down_y, far_y = ring(cy, 1, ny), ring(cy, -1, ny), ring(cy, 2, ny)

    def zx_forward():
        got(xv, sem("zx", 0))
        got(means.at[0], sem("mean", 0))
        spread(2)
        normalise(2, cy)
        send(zb(2, 0, lo), zb(2, 0, lo), dev(dx=1), sem("zx", 2), z_sends)
        zy_send(2)
        got(xv, sem("zx", 1))
        got(means.at[0], sem("mean", 1))
        spread(1)
        normalise(1, cy)
        send(zb(1, 0, hi), zb(1, 0, hi), dev(dx=-1), sem("zx", 3), z_sends)
        zy_send(1)

    def zx_last():
        got(zb(3, 0, lo), sem("zx", 2))
        got(zb(3, 0, hi), sem("zx", 3))

    def zy_send(b):
        send(zb(b, 0), zb(b, 0), dev(dy=1), sem("zy", 4 * b), z_sends)
        send(zb(b, 0), zb(b, 0), dev(dy=-1), sem("zy", 4 * b + 1), z_sends)

    def zy_forward(b):
        got(zb(b, -1), sem("zy", 4 * b))
        send(zb(b, -1, lo), zb(b, -1, lo), dev(dy=1), sem("zy", 4 * b + 2), z_sends)
        got(zb(b, 1), sem("zy", 4 * b + 1))
        send(zb(b, 1, hi), zb(b, 1, hi), dev(dy=-1), sem("zy", 4 * b + 3), z_sends)

    def zy_last(b):
        got(zb(b, 2, lo), sem("zy", 4 * b + 2))
        got(zb(b, 2, hi), sem("zy", 4 * b + 3))

    def zy_forward_own():
        got(xv, sem("zy", 0))
        for d in range(1, ny):
            got(gains.at[0], sem("gain", d - 1))
        normalise(0, down_y)
        send(zb(0, -1, lo), zb(0, -1, lo), dev(dy=1), sem("zy", 2), z_sends)
        got(xv, sem("zy", 1))
        normalise(0, up_y)
        send(zb(0, 1, hi), zb(0, 1, hi), dev(dy=-1), sem("zy", 3), z_sends)

    def wt_rows(t, slot, rows):
        for j in rows:
            for core in range(2):
                r = 2 * ring(cx, j, nx) + lax.rem(k + core, 2)
                dst = wt.at[slot, r // 2, pl.ds(pl.multiple_of(lax.rem(r, 2) * krows, krows), krows)]
                src = win.at[:, columns(0, t)] if j == 0 and core == 0 else w_hbm.at[t, r]
                pltpu.make_async_copy(src, dst, ls.at[1 + slot]).start()

    def wt_load(t, slot):
        wt_rows(t, slot, range(nx))

    def wt_wait(slot):
        pltpu.make_async_copy(wt.at[slot], wt.at[slot], ls.at[1 + slot]).wait()

    def up_load(t0, t1):
        for i in range(min(2, t1 - t0)):
            wt_load(t0 + i, i)

    def up(late, t0, t1, b0, b1, loaded=False):
        hm, hf, first = (hm_b, hf_b, early) if late else (hm_a, hf_a, 0)
        if not loaded:
            up_load(t0, t1)

        def tile(i, _):
            slot = lax.rem(i, 3)
            wt_wait(slot)

            @pl.when(i + 2 < t1 - t0)
            def _():
                wt_load(t0 + i + 2, lax.rem(i + 2, 3))

            at = pl.ds(pl.multiple_of((t0 + i - first) * tw, 128), tw)

            def rows(b, _):
                t = ring(cx, b + b // 2 - 2 * (b // 3), nx)
                v = jnp.dot(z[t, 0], wt[slot, 0], preferred_element_type=jnp.float32)
                for j in range(1, ny):
                    v += jnp.dot(z[t, j], wt[slot, j], preferred_element_type=jnp.float32)
                hm[t, :, :, :, at] = gelu(v).astype(hm.dtype).reshape(ny, SUB, piece, tw)

                @pl.when(cx == cy)
                def _():
                    hf[0, :, t, cy, :, at] = hm[t, cy, :, :, at]

                return 0

            lax.fori_loop(b0, b1, rows, 0)
            return 0

        lax.fori_loop(0, t1 - t0, tile, 0)

    def up_near(t):
        got(w_hbm.at[t, row], sem("wo", t))
        w_got(t, (1, 3))
        wt_rows(t, 0, (0, 1, 3))
        ref = wt.at[0, pl.ds(0, ny - 1)]
        pltpu.make_async_copy(ref, ref, ls.at[1]).wait()

        def rows(b, _):
            v = None
            for j in (0, 1, 3):
                f = ring(cx, j, nx)
                p = jnp.dot(z[b, f], wt[0, f], preferred_element_type=jnp.float32)
                v = p if v is None else v + p
            pre[b] = v
            return 0

        lax.fori_loop(0, nx, rows, 0)

    def up_far(t):
        w_got(t, (2,))
        wt_rows(t, 0, (2,))
        f = ring(cx, 2, nx)
        pltpu.make_async_copy(wt.at[0, f], wt.at[0, f], ls.at[1]).wait()
        at = pl.ds((t - early) * tw, tw)

        def rows(b, _):
            v = pre[b] + jnp.dot(z[b, f], wt[0, f], preferred_element_type=jnp.float32)
            hm_b[b, :, :, :, at] = gelu(v).astype(hm_b.dtype).reshape(ny, SUB, piece, tw)

            @pl.when(cx == cy)
            def _():
                hf_b[0, :, b, cy, :, at] = hm_b[b, cy, :, :, at]

            return 0

        lax.fori_loop(0, nx, rows, 0)

    def h1_a(b):
        t = ring(cx, off[b], nx)
        for d in (1, 3, 2):
            c = ring(cy, d, ny)
            i = sem("h1a", 3 * b + d - 1)

            @pl.when(cx == cy)
            def _():
                remote(hm_a.at[t, c], hf_a.at[0, :, t, c], dev(dy=d), i).start()

            @pl.when(cx != cy)
            def _():
                remote(hm_a.at[t, c], hst_a.at[cy, :, t], dev(dy=d), i).start()

            sends.append(remote(hm_a.at[t, c], hst_a.at[cy, :, t], dev(dy=d), i))

    def h1_wait(b):
        for d in range(1, ny):
            got(hst_a.at[0, :, 0], sem("h1a", 3 * b + d - 1))

    def h2_a(b, g):
        t = ring(cx, off[b], nx)
        some = pl.ds(g * batch, batch)
        for d in (1, 3, 2):
            c = ring(cx, d, nx)
            i = sem("h2a", 12 * g + 3 * b + d - 1)

            @pl.when(c == cy)
            def _():
                remote(hm_a.at[t, cy, some], hf_a.at[nx - d, some, t, cy], dev(dx=d), i).start()

            @pl.when(c != cy)
            def _():
                remote(hst_a.at[c, some, t], hf_a.at[nx - d, some, t, cy], dev(dx=d), i).start()

            sends.append(remote(hst_a.at[c, some, t], hf_a.at[nx - d, some, t, cy], dev(dx=d), i))

    def h1_b(s):
        for d in (1, 3, 2):
            c = ring(cy, d, ny)
            i = sem("h1b", 3 * s + d - 1)

            @pl.when(cx == cy)
            def _():
                remote(hm_b.at[:, c, s], hf_b.at[0, s, :, c], dev(dy=d), i).start()

            @pl.when(cx != cy)
            def _():
                remote(hm_b.at[:, c, s], hst_b.at[cy, s], dev(dy=d), i).start()

            sends.append(remote(hm_b.at[:, c, s], hst_b.at[cy, s], dev(dy=d), i))

    def h2_b(s):
        for d in range(1, ny):
            got(hst_b.at[0, 0], sem("h1b", 3 * s + d - 1))
        for d in (1, 3, 2):
            c = ring(cx, d, nx)
            i = sem("h2b", 3 * s + d - 1)

            @pl.when(c == cy)
            def _():
                remote(hm_b.at[:, cy, s], hf_b.at[nx - d, s, :, cy], dev(dx=d), i).start()

            @pl.when(c != cy)
            def _():
                remote(hst_b.at[c, s], hf_b.at[nx - d, s, :, cy], dev(dx=d), i).start()

            sends.append(remote(hst_b.at[c, s], hf_b.at[nx - d, s, :, cy], dev(dx=d), i))

    def gather(i, whole, low, high):
        def begin():
            send(whole(cy), whole(cy), dev(dy=1), i)
            send(whole(cy), whole(cy), dev(dy=-1), i + 1)

        def forward():
            got(whole(cy), i)
            send(low(down_y), low(down_y), dev(dy=1), i + 2)
            got(whole(cy), i + 1)
            send(high(up_y), high(up_y), dev(dy=-1), i + 3)

        def last():
            got(low(far_y), i + 2)
            got(high(far_y), i + 3)

        return begin, forward, last

    def gather_own(b):
        t = ring(cx, off[b], nx)
        part = lambda s, n: lambda y: hf_a.at[0, pl.ds(s, n), t, y]
        return gather(sem("own", 4 * b), part(0, SUB), part(0, SUB // 2), part(SUB // 2, SUB // 2))

    def gather_a(g):
        part = lambda s, n: lambda y: hf_a.at[pl.ds(1, nx - 1), pl.ds(g * batch + s, n), :, y]
        return gather(sem("aga", 4 * g), part(0, batch), part(0, batch // 2), part(batch // 2, batch // 2))

    def gather_b(s):
        part = lambda c, n: lambda y: hf_b.at[pl.ds(c, n), s, :, y]
        return gather(sem("agb", 4 * s), part(0, nx), part(0, nx // 2), part(nx // 2, nx // 2))

    own_gathers = [gather_own(b) for b in range(nx)]
    a_gathers = [gather_a(g) for g in range(GROUPS)]
    b_gathers = [gather_b(s) for s in range(SUB)]

    def own_a(b):
        own_gathers[b][0]()

    def own_a_forward(b):
        own_gathers[b][1]()

    def own_a_last(b):
        own_gathers[b][2]()

    def ag_a(g):
        for j in range(12):
            got(hst_a.at[0, pl.ds(0, batch), 0], sem("h2a", 12 * g + j))
        a_gathers[g][0]()

    def ag_a_forward(g):
        a_gathers[g][1]()

    def ag_a_last(g):
        a_gathers[g][2]()

    def ag_b(s):
        for d in range(1, nx):
            got(hst_b.at[0, 0], sem("h2b", 3 * s + d - 1))
        b_gathers[s][0]()

    def ag_b_forward(s):
        b_gathers[s][1]()

    def ag_b_last(s):
        b_gathers[s][2]()

    ew, lw = early * tw, LATE * tw
    npt = 2 * krows // ew
    steps = dloc // (npt * tw)
    kept = lw // tok

    def rows_of(c, skip, count, use):
        at = pl.ds(pl.multiple_of(lax.rem(c, 2) * (ew + lw) + skip, 128), count)

        @pl.when(c // 2 == k)
        def _():
            use(wout, at)

        @pl.when(c // 2 != k)
        def _():
            use(wo_hbm, at)

    def we_load(i, slot):
        for j in range(npt):
            for p in range(nx):
                cols = pl.ds(pl.multiple_of((i * npt + j) * tw, 128), tw)
                dst = wt.at[slot, p, pl.ds(j * ew, ew)]
                rows_of(ring(cx, p, nx), 0, ew, lambda ref, at: pltpu.make_async_copy(ref.at[at, cols], dst, ls.at[1 + slot]).start())

    def we_wait(slot):
        ref = wt.at[slot, :, pl.ds(0, npt * ew)]
        pltpu.make_async_copy(ref, ref, ls.at[1 + slot]).wait()

    def down_early_load():
        for i in range(min(2, steps)):
            we_load(i, i)

    def down_early(g, loaded=False):
        some = pl.ds(g * batch, batch)
        if not loaded:
            down_early_load()

        def step(i, _):
            slot = lax.rem(i, 3)
            we_wait(slot)

            @pl.when(i + 2 < steps)
            def _():
                we_load(i + 2, lax.rem(i + 2, 3))

            for j in range(npt):
                v = None
                for p in range(nx):
                    h = hf_a[p, some].reshape(batch * nx * sub, ew)
                    w = jnp.dot(h, wt[slot, p, pl.ds(j * ew, ew)], preferred_element_type=jnp.float32)
                    v = w if v is None else v + w
                cols = pl.ds(pl.multiple_of((i * npt + j) * tw, 128), tw)
                acc[some, :, :, cols] = v.reshape(batch, nx, sub, tw)
            return 0

        lax.fori_loop(0, steps, step, 0)

    def late_start():
        for c in z_sends:
            c.wait_send()
        for p in range(nx):
            for j in range(kept):
                rows_of(ring(cx, p, nx), ew + j * tok, tok, lambda ref, at: pltpu.make_async_copy(ref.at[at], z.at[p, j], ls.at[4]).start())

    def late_wait():
        ref = z.at[:, pl.ds(0, kept)]
        pltpu.make_async_copy(ref, ref, ls.at[4]).wait()

    def down_late(s):
        wide = 2 * tw

        def step(i, _):
            cols = pl.ds(pl.multiple_of(i * wide, 128), wide)
            v = None
            for c in range(nx):
                h = hf_b[c, s].reshape(nx * sub, lw)
                p = jnp.dot(h, z[c, pl.ds(0, kept), :, cols].reshape(lw, wide), preferred_element_type=jnp.float32)
                v = p if v is None else v + p
            acc[s, :, :, cols] += v.reshape(nx, sub, wide)
            return 0

        lax.fori_loop(0, dloc // wide, step, 0)

    top, low = pl.ds(0, sub // 2), pl.ds(sub // 2, sub // 2)
    right, left, across = ring(cx, 1, nx), ring(cx, -1, nx), ring(cx, 2, nx)

    def y_send(s):
        send(acc.at[s, across, top], ya.at[s, 0], dev(dx=1), sem("y", 6 * s))
        send(acc.at[s, across, low], ya.at[s, 1], dev(dx=-1), sem("y", 6 * s + 1))
        send(acc.at[s, right, low], yb.at[s, 0, low], dev(dx=1), sem("y", 6 * s + 2))
        send(acc.at[s, left, top], yb.at[s, 1, top], dev(dx=-1), sem("y", 6 * s + 3))

    def y_forward(s):
        got(ya.at[s, 0], sem("y", 6 * s))
        acc[s, right, top] += ya[s, 0]
        send(acc.at[s, right, top], yb.at[s, 0, top], dev(dx=1), sem("y", 6 * s + 4))
        got(ya.at[s, 1], sem("y", 6 * s + 1))
        acc[s, left, low] += ya[s, 1]
        send(acc.at[s, left, low], yb.at[s, 1, low], dev(dx=-1), sem("y", 6 * s + 5))

    def y_final(s):
        for j in range(2, 6):
            got(ya.at[s, 0], sem("y", 6 * s + j))
        for c in range(ny):
            rows, at = pl.ds(c * piece, piece), pl.ds(c * (tok // ny) + s * piece, piece)
            total = acc[s, cx, rows] + (yb[s, 0, rows] + yb[s, 1, rows])
            ov[at, :] = (xv[at, :].astype(jnp.float32) + total).astype(ov.dtype)

    n0, n1, n2, n3, n4, n5, n6, n7 = range(8)
    yes = True
    w_issue(n1)
    zy_forward_own()
    zx_forward()
    w_issue(n2)
    w_issue(n3)
    w_forward(n0)
    zy_forward(n2)
    zy_last(n0)
    w_forward(n1)
    got(wo_hbm, sem("wout"))
    w_ready(n1)
    up(n0, n1, n2, n0, n1)
    zx_last()
    w_issue(n4)
    zy_send(n3)
    w_ready(n0)
    up(n0, n0, n1, n0, n1)
    zy_forward(n1)
    w_forward(n2)
    zy_last(n2)
    w_issue(n5)
    w_ready(n2)
    up(n0, n0, n3, n2, n3)
    zy_forward(n3)
    w_forward(n3)
    zy_last(n1)
    w_ready(n3)
    up(n0, n3, n4, n0, n3)
    up_load(n0, n3)
    h1_a(n2)
    up(n0, n0, n3, n1, n2, yes)
    up_load(n2, n3)
    h1_a(n1)
    h1_wait(n2)
    own_a(n2)
    zy_last(n3)
    up(n0, n2, n3, n0, n1, yes)
    up_load(n0, n4)
    h1_a(n0)
    up(n0, n0, n4, n3, n4, yes)
    h1_wait(n1)
    h2_a(n1, n0)
    h1_a(n3)
    own_a(n1)
    h1_wait(n0)
    own_a(n0)
    h2_a(n2, n0)
    h2_a(n0, n0)
    h1_wait(n3)
    h2_a(n3, n0)
    h2_a(n2, n1)
    h2_a(n2, n2)
    own_a_forward(n2)
    w_forward(n4)
    h2_a(n3, n1)
    own_a(n3)
    h2_a(n3, n2)
    own_a_forward(n1)
    h2_a(n0, n1)
    w_forward(n5)
    own_a_forward(n0)
    h2_a(n1, n1)
    h2_a(n1, n2)
    ag_a(n0)
    h2_a(n0, n2)
    w_ready(n5)
    up(n1, n5, n6, n0, n4)
    w_issue(n6)
    own_a_forward(n3)
    ag_a(n1)
    ag_a(n2)
    w_ready(n4)
    up(n1, n4, n5, n0, n4)
    own_a_last(n3)
    ag_a_forward(n0)
    ag_a_forward(n1)
    own_a_last(n1)
    w_forward_near(n6)
    h2_a(n3, n3)
    up_near(n6)
    own_a_last(n0)
    w_forward_far(n6)
    ag_a_last(n0)
    ag_a_forward(n2)
    up_far(n6)
    down_early_load()
    h1_b(n0)
    h1_b(n1)
    h1_b(n2)
    h1_b(n3)
    own_a_last(n2)
    h2_a(n0, n3)
    h1_b(n4)
    ag_a_last(n2)
    h2_b(n0)
    h1_b(n5)
    down_early(n0, yes)
    down_early_load()
    ag_b(n0)
    h2_b(n1)
    h2_b(n2)
    h2_b(n3)
    h1_b(n6)
    h2_a(n1, n3)
    ag_b(n1)
    h2_b(n4)
    h2_b(n5)
    ag_b_forward(n0)
    ag_a_last(n1)
    late_start()
    h2_a(n2, n3)
    ag_b(n2)
    down_early(n1, yes)
    down_early_load()
    ag_b_forward(n1)
    h2_b(n6)
    ag_b(n3)
    ag_b_last(n0)
    h1_b(n7)
    late_wait()
    down_late(n0)
    y_send(n0)
    ag_b_forward(n2)
    ag_b(n4)
    ag_b_last(n1)
    down_late(n1)
    y_send(n1)
    y_forward(n0)
    down_early(n2, yes)
    down_early_load()
    ag_b_last(n2)
    ag_b(n5)
    h2_b(n7)
    down_late(n2)
    y_send(n2)
    ag_b_forward(n3)
    ag_b_forward(n4)
    ag_b_forward(n5)
    y_forward(n2)
    ag_a(n3)
    ag_b_last(n3)
    down_late(n3)
    y_send(n3)
    ag_b(n6)
    ag_b_last(n4)
    ag_b_last(n5)
    down_late(n4)
    y_send(n4)
    y_final(n2)
    down_late(n5)
    y_send(n5)
    y_forward(n1)
    ag_a_forward(n3)
    y_forward(n5)
    y_forward(n4)
    ag_b_forward(n6)
    y_forward(n3)
    ag_b(n7)
    ag_a_last(n3)
    down_early(n3, yes)
    ag_b_last(n6)
    down_late(n6)
    y_send(n6)
    ag_b_forward(n7)
    y_final(n5)
    y_final(n1)
    y_forward(n6)
    ag_b_last(n7)
    down_late(n7)
    y_send(n7)
    y_final(n6)
    y_final(n3)
    y_final(n0)
    y_final(n4)
    y_forward(n7)
    y_final(n7)
    out = pltpu.make_async_copy(ov, y_hbm, ls.at[0])
    out.start()
    for c in sends:
        c.wait_send()
    out.wait()


def solution(mesh):
    nx, ny = mesh.shape["row"] // 2, mesh.shape["col"]

    def local_block(x, gain, win, wout):
        tok, dloc = x.shape
        krows, floc = win.shape
        width = floc // nx
        tw = width // 7
        tiles = width // tw
        early = tiles - LATE
        ew, lw = early * tw, LATE * tw
        sub = tok // SUB
        piece = sub // ny
        bf, f32 = jnp.bfloat16, jnp.float32
        count = plan(tiles).total
        hbm = lambda shape, dt: jax.ShapeDtypeStruct(shape, dt)
        outs = pl.pallas_call(
            functools.partial(block, (nx, ny, dloc * ny)),
            name="mlp_block",
            out_shape=[
                hbm((tok, dloc), bf),
                hbm((tiles, 2 * nx, krows, tw), bf),
                hbm(wout.shape, bf),
                hbm((ny, SUB, nx, piece, ew), bf),
                hbm((ny, SUB, nx, piece, lw), bf),
            ],
            in_specs=[
                pl.BlockSpec(memory_space=pl.ANY),
                pl.BlockSpec(memory_space=pltpu.VMEM),
                pl.BlockSpec(memory_space=pl.ANY),
                pl.BlockSpec(memory_space=pl.ANY),
            ],
            out_specs=[pl.BlockSpec(memory_space=pl.ANY)] * 5,
            scratch_shapes=[
                pltpu.VMEM((tok, dloc), bf),
                pltpu.VMEM((3, tok, 128), f32),
                pltpu.VMEM((ny, 8, tok), f32),
                pltpu.VMEM((3, 8, tok), f32),
                pltpu.VMEM((ny, 1, dloc), f32),
                pltpu.VMEM((nx, ny, tok, dloc), bf),
                pltpu.VMEM((3, ny, 2 * krows, tw), bf),
                pltpu.VMEM((nx, ny, SUB, piece, ew), bf),
                pltpu.VMEM((nx, ny, SUB, piece, lw), bf),
                pltpu.VMEM((nx, SUB, nx, ny, piece, ew), bf),
                pltpu.VMEM((nx, SUB, nx, ny, piece, lw), bf),
                pltpu.VMEM((SUB, nx, sub, dloc), f32),
                pltpu.VMEM((nx, tok, tw), f32),
                pltpu.VMEM((SUB, 2, sub // 2, dloc), f32),
                pltpu.VMEM((SUB, 2, sub, dloc), f32),
                pltpu.VMEM((tok, dloc), bf),
                pltpu.SemaphoreType.DMA((count,)),
                pltpu.SemaphoreType.DMA((count,)),
                pltpu.SemaphoreType.DMA((5,)),
            ],
            compiler_params=pltpu.CompilerParams(
                collective_id=0, has_side_effects=True, vmem_limit_bytes=67043328
            ),
        )(x, gain.reshape(1, dloc), win, wout)
        return outs[0]

    return jax.shard_map(
        local_block,
        mesh=mesh,
        in_specs=(P(("dp", "row"), "col"), P("col"), P("row", "col"), P("row", "col")),
        out_specs=P(("dp", "row"), "col"),
        check_vma=False,
    )
```

```python
import functools

import jax
import jax.numpy as jnp
from jax import lax
from jax.experimental import pallas as pl
from jax.experimental.pallas import tpu as pltpu
from jax.sharding import PartitionSpec as P

NORM_EPS = 1e-5
MESH = pl.DeviceIdType.MESH
NEAR_FIRST = (1, 3, 2)
SUB = 8
GROUPS = 4
LATE = 3


def gelu(v):
    return 0.5 * v * (1.0 + jnp.tanh(0.7978845608028654 * (v + 0.044715 * (v * v * v))))


KINDS = (
    "stat", "gain", "mean", "raw", "zf", "zy", "w", "pair", "wout", "h1a", "h2a", "h1b", "h2b", "own", "aga", "agb", "y",
)


class Sems:
    def __init__(self):
        self.base, self.total = {}, 0

    def add(self, name, count):
        self.base[name] = self.total
        self.total += count

    def __call__(self, name, index=0):
        return self.base[name] + index


def plan(tiles):
    s = Sems()
    for name, count in (
        ("stat", 1), ("gain", 1), ("mean", 2), ("zx", 4), ("zy", 16), ("rest", 4), ("w", 3 * tiles), ("wf", tiles + 1),
        ("wout", 1), ("h1a", 4), ("h1b", SUB), ("h2a", GROUPS), ("h2b", SUB),
        ("own", 12), ("aga", 3 * GROUPS), ("agb", 3 * SUB), ("y", 3 * SUB),
    ):
        s.add(name, count)
    return s


def block(n, x_hbm, gain_ref, win, wout, ov, w_hbm, wo_hbm, hst_a, hst_b,
          xv, sums, stat, means, gains, z, wt, hm_a, hm_b, hf_a, hf_b, acc, pre, ya, yb, ss, rs, ls):
    nx, ny, d_model = n
    row, cy = lax.axis_index("row"), lax.axis_index("col")
    cx, k = row // 2, lax.rem(row, 2)
    tok, dloc = ov.shape
    tiles, krows, tw = w_hbm.shape[0], w_hbm.shape[2], w_hbm.shape[3]
    early = tiles - LATE
    half = tok // 2
    sub = tok // SUB
    piece = sub // ny
    batch = SUB // GROUPS
    sem = plan(tiles)

    def ring(v, d, m):
        return lax.rem(v + (d + m), m)

    def dev(dx=0, dy=0, core=None):
        return {"row": 2 * ring(cx, dx, nx) + (k if core is None else core), "col": ring(cy, dy, ny)}

    partner = dev(core=1 - k)

    def remote(src, dst, where, i, kind):
        return pltpu.make_async_remote_copy(
            src_ref=src, dst_ref=dst, send_sem=ss.at[KINDS.index(kind)], recv_sem=rs.at[i], device_id=where, device_id_type=MESH
        )

    def send(src, dst, where, i, kind):
        remote(src, dst, where, i, kind).start()

    def got(ref, i):
        remote(ref, ref, partner, i, "w").wait_recv()

    def drain(kind, ref):
        remote(ref, ref, partner, 0, kind).wait_send()

    barrier = pltpu.get_barrier_semaphore()
    peers = [partner] + [dev(dx=d) for d in range(1, nx)] + [dev(dy=d) for d in range(1, ny)]
    for p in peers:
        pl.semaphore_signal(barrier, inc=1, device_id=p, device_id_type=MESH)
    load_x = pltpu.make_async_copy(x_hbm, xv, ls.at[0])
    load_x.start()
    pl.semaphore_wait(barrier, len(peers))

    off = (0, 1, 3, 2)
    lo, hi = pl.ds(0, half), pl.ds(half, half)

    def zb(b, dy, rows=None):
        ref = z.at[ring(cx, off[b], nx), ring(cy, dy, ny)]
        return ref if rows is None else ref.at[rows]

    def raw(rows, where, i):
        send(x_hbm.at[rows], zb(0, 0, rows), where, i, "raw")

    raw(lo, dev(dy=1), sem("zy", 0))
    raw(hi, dev(dy=-1), sem("zy", 1))
    raw(lo, dev(dx=1), sem("zx", 0))
    raw(hi, dev(dx=-1), sem("zx", 1))
    load_x.wait()

    lane = lax.broadcasted_iota(jnp.int32, (32, sums.shape[2]), 1)

    def part(i, _):
        at = pl.ds(pl.multiple_of(i * 32, 32), 32)
        v = xv[at, :].astype(jnp.float32)
        s1 = jnp.sum(v, axis=1, keepdims=True)
        s2 = jnp.sum(v * v, axis=1, keepdims=True)
        sums[0, at, :] = jnp.where(lane == 0, s1, s2)
        return 0

    lax.fori_loop(0, tok // 32, part, 0)
    stat[cy] = jnp.transpose(sums[0])[: stat.shape[1]]
    gains[cy] = gain_ref[...]
    for d in NEAR_FIRST:
        send(stat.at[cy], stat.at[cy], dev(dy=d), sem("stat"), "stat")
    for d in NEAR_FIRST:
        send(gains.at[cy], gains.at[cy], dev(dy=d), sem("gain"), "gain")
    raw(hi, dev(dy=1), sem("rest", 0))
    raw(lo, dev(dy=-1), sem("rest", 1))
    raw(hi, dev(dx=1), sem("rest", 2))
    raw(lo, dev(dx=-1), sem("rest", 3))

    def columns(dx, t):
        return pl.ds(pl.multiple_of(ring(cx, dx, nx) * (tiles * tw) + t * tw, 128), tw)

    last = tiles - 1

    def w_issue(t):
        for d in NEAR_FIRST:
            send(win.at[:, columns(d, t)], w_hbm.at[t, row], dev(dx=d), sem("w", 3 * t + d - 1), "w")
        send(win.at[:, columns(0, t)], w_hbm.at[t, row], partner, sem("wf", t), "pair")

    def w_pass(t, ds):
        for d in ds:
            slot = 2 * ring(cx, -d, nx) + k
            got(w_hbm.at[t, slot], sem("w", 3 * t + d - 1))
            i = sem("wf", tiles if t == last and d == NEAR_FIRST[-1] else t)
            send(w_hbm.at[t, slot], w_hbm.at[t, slot], partner, i, "pair")

    def w_forward(t):
        w_pass(t, NEAR_FIRST)

    def w_ready(t):
        got(w_hbm.at[t, pl.ds(0, nx)], sem("wf", t))

    def w_forward_near(t):
        w_pass(t, NEAR_FIRST[:-1])

    def w_forward_far(t):
        w_pass(t, NEAR_FIRST[-1:])

    got(stat.at[pl.ds(0, ny - 1)], sem("stat"))
    total = (stat[0] + stat[1]) + (stat[2] + stat[3])
    mean = total[0:1] / d_model
    rstd = lax.rsqrt(total[1:2] / d_model - mean * mean + NORM_EPS)
    means[0] = jnp.where(lax.broadcasted_iota(jnp.int32, total.shape, 0) == 0, mean, rstd)
    send(means.at[0], means.at[2], dev(dx=1), sem("mean", 0), "mean")
    send(means.at[0], means.at[1], dev(dx=-1), sem("mean", 1), "mean")
    w_issue(0)
    send(wout, wo_hbm, partner, sem("wout"), "wout")

    def spread(b):
        copies = sums.shape[2] // means.shape[1]
        sums[b] = jnp.transpose(jnp.concatenate([means[b]] * copies, axis=0))

    def normalise(b, y, src=None, r0=0, r1=tok):
        t = ring(cx, off[b], nx)

        def norm(i, _):
            at = pl.ds(pl.multiple_of(i * 32, 32), 32)
            v = (z[t, y, at, :] if src is None else src[at, :]).astype(jnp.float32)
            z[t, y, at, :] = ((v - sums[b, at, 0:1]) * sums[b, at, 1:2] * gains[y]).astype(z.dtype)
            return 0

        lax.fori_loop(r0 // 32, r1 // 32, norm, 0)

    spread(0)
    normalise(0, cy, xv)

    up_y, down_y, far_y = ring(cy, 1, ny), ring(cy, -1, ny), ring(cy, 2, ny)

    def zx_forward():
        got(zb(2, 0, lo), sem("zx", 0))
        got(means.at[0], sem("mean", 0))
        got(zb(2, 0, hi), sem("rest", 2))
        spread(2)
        normalise(2, cy)
        send(zb(2, 0, lo), zb(2, 0, lo), dev(dx=1), sem("zx", 2), "zf")
        zy_send(2)
        got(zb(1, 0, hi), sem("zx", 1))
        got(means.at[0], sem("mean", 1))
        got(zb(1, 0, lo), sem("rest", 3))
        spread(1)
        normalise(1, cy)
        send(zb(1, 0, hi), zb(1, 0, hi), dev(dx=-1), sem("zx", 3), "zf")
        zy_send(1)

    def zx_last():
        got(zb(3, 0, lo), sem("zx", 2))
        got(zb(3, 0, hi), sem("zx", 3))

    def zy_send(b):
        send(zb(b, 0), zb(b, 0), dev(dy=1), sem("zy", 4 * b), "zy")
        send(zb(b, 0), zb(b, 0), dev(dy=-1), sem("zy", 4 * b + 1), "zy")

    def zy_forward(b):
        got(zb(b, -1), sem("zy", 4 * b))
        send(zb(b, -1, lo), zb(b, -1, lo), dev(dy=1), sem("zy", 4 * b + 2), "zy")
        got(zb(b, 1), sem("zy", 4 * b + 1))
        send(zb(b, 1, hi), zb(b, 1, hi), dev(dy=-1), sem("zy", 4 * b + 3), "zy")

    def zy_last(b):
        got(zb(b, 2, lo), sem("zy", 4 * b + 2))
        got(zb(b, 2, hi), sem("zy", 4 * b + 3))

    def zy_own_near():
        got(gains.at[pl.ds(0, ny - 1)], sem("gain"))
        got(zb(0, -1, lo), sem("zy", 0))
        normalise(0, down_y, None, 0, half)
        send(zb(0, -1, lo), zb(0, -1, lo), dev(dy=1), sem("zy", 2), "zf")
        got(zb(0, 1, hi), sem("zy", 1))
        normalise(0, up_y, None, half, tok)
        send(zb(0, 1, hi), zb(0, 1, hi), dev(dy=-1), sem("zy", 3), "zf")

    def zy_own_rest():
        got(zb(0, -1, hi), sem("rest", 0))
        normalise(0, down_y, None, half, tok)
        got(zb(0, 1, lo), sem("rest", 1))
        normalise(0, up_y, None, 0, half)

    def wt_rows(t, slot, rows):
        for j in rows:
            for core in range(2):
                r = 2 * ring(cx, j, nx) + lax.rem(k + core, 2)
                dst = wt.at[slot, r // 2, pl.ds(pl.multiple_of(lax.rem(r, 2) * krows, krows), krows)]
                src = win.at[:, columns(0, t)] if j == 0 and core == 0 else w_hbm.at[t, r]
                pltpu.make_async_copy(src, dst, ls.at[1 + slot]).start()

    def wt_load(t, slot):
        wt_rows(t, slot, range(nx))

    def wt_wait(slot):
        pltpu.make_async_copy(wt.at[slot], wt.at[slot], ls.at[1 + slot]).wait()

    def up_load(t0, t1):
        for i in range(min(2, t1 - t0)):
            wt_load(t0 + i, i)

    def up(late, t0, t1, b0, b1, loaded=False):
        hm, hf, first = (hm_b, hf_b, early) if late else (hm_a, hf_a, 0)
        if not loaded:
            up_load(t0, t1)

        def tile(i, _):
            slot = lax.rem(i, 3)
            wt_wait(slot)

            @pl.when(i + 2 < t1 - t0)
            def _():
                wt_load(t0 + i + 2, lax.rem(i + 2, 3))

            at = pl.ds(pl.multiple_of((t0 + i - first) * tw, 128), tw)

            def rows(b, _):
                t = ring(cx, b + b // 2 - 2 * (b // 3), nx)
                v = jnp.dot(z[t, 0], wt[slot, 0], preferred_element_type=jnp.float32)
                for j in range(1, ny):
                    v += jnp.dot(z[t, j], wt[slot, j], preferred_element_type=jnp.float32)
                hm[t, :, :, :, at] = gelu(v).astype(hm.dtype).reshape(ny, SUB, piece, tw)

                @pl.when(cx == cy)
                def _():
                    hf[0, :, t, cy, :, at] = hm[t, cy, :, :, at]

                return 0

            lax.fori_loop(b0, b1, rows, 0)
            return 0

        lax.fori_loop(0, t1 - t0, tile, 0)

    def up_near(t):
        got(w_hbm.at[t, pl.ds(0, nx - 1)], sem("wf", t))
        wt_rows(t, 0, (0, 1, 3))
        ref = wt.at[0, pl.ds(0, ny - 1)]
        pltpu.make_async_copy(ref, ref, ls.at[1]).wait()

        def rows(b, _):
            v = None
            for j in (0, 1, 3):
                f = ring(cx, j, nx)
                p = jnp.dot(z[b, f], wt[0, f], preferred_element_type=jnp.float32)
                v = p if v is None else v + p
            pre[b] = v
            return 0

        lax.fori_loop(0, nx, rows, 0)

    def up_far(t):
        got(w_hbm.at[t, row], sem("wf", tiles))
        wt_rows(t, 0, (2,))
        f = ring(cx, 2, nx)
        pltpu.make_async_copy(wt.at[0, f], wt.at[0, f], ls.at[1]).wait()
        at = pl.ds((t - early) * tw, tw)

        def rows(b, _):
            v = pre[b] + jnp.dot(z[b, f], wt[0, f], preferred_element_type=jnp.float32)
            hm_b[b, :, :, :, at] = gelu(v).astype(hm_b.dtype).reshape(ny, SUB, piece, tw)

            @pl.when(cx == cy)
            def _():
                hf_b[0, :, b, cy, :, at] = hm_b[b, cy, :, :, at]

            return 0

        lax.fori_loop(0, nx, rows, 0)

    def h1_a(b):
        t = ring(cx, off[b], nx)
        for d in NEAR_FIRST:
            c = ring(cy, d, ny)
            i = sem("h1a", b)

            @pl.when(cx == cy)
            def _():
                remote(hm_a.at[t, c], hf_a.at[0, :, t, c], dev(dy=d), i, "h1a").start()

            @pl.when(cx != cy)
            def _():
                remote(hm_a.at[t, c], hst_a.at[cy, :, t], dev(dy=d), i, "h1a").start()

    def h1_wait(b):
        got(hst_a.at[pl.ds(0, ny - 1), :, 0], sem("h1a", b))

    def h2_a(b, g):
        t = ring(cx, off[b], nx)
        some = pl.ds(g * batch, batch)
        for d in NEAR_FIRST:
            c = ring(cx, d, nx)
            i = sem("h2a", g)

            @pl.when(c == cy)
            def _():
                remote(hm_a.at[t, cy, some], hf_a.at[nx - d, some, t, cy], dev(dx=d), i, "h2a").start()

            @pl.when(c != cy)
            def _():
                remote(hst_a.at[c, some, t], hf_a.at[nx - d, some, t, cy], dev(dx=d), i, "h2a").start()

    def h1_b(s):
        for d in NEAR_FIRST:
            c = ring(cy, d, ny)
            i = sem("h1b", s)

            @pl.when(cx == cy)
            def _():
                remote(hm_b.at[:, c, s], hf_b.at[0, s, :, c], dev(dy=d), i, "h1b").start()

            @pl.when(cx != cy)
            def _():
                remote(hm_b.at[:, c, s], hst_b.at[cy, s], dev(dy=d), i, "h1b").start()

    def h2_b(s):
        got(hst_b.at[pl.ds(0, ny - 1), 0], sem("h1b", s))
        for d in NEAR_FIRST:
            c = ring(cx, d, nx)
            i = sem("h2b", s)

            @pl.when(c == cy)
            def _():
                remote(hm_b.at[:, cy, s], hf_b.at[nx - d, s, :, cy], dev(dx=d), i, "h2b").start()

            @pl.when(c != cy)
            def _():
                remote(hst_b.at[c, s], hf_b.at[nx - d, s, :, cy], dev(dx=d), i, "h2b").start()

    def gather(kind, i, whole, low, high):
        def begin():
            send(whole(cy), whole(cy), dev(dy=1), i, kind)
            send(whole(cy), whole(cy), dev(dy=-1), i + 1, kind)

        def forward():
            got(whole(cy), i)
            send(low(down_y), low(down_y), dev(dy=1), i + 2, kind)
            got(whole(cy), i + 1)
            send(high(up_y), high(up_y), dev(dy=-1), i + 2, kind)

        def last():
            got(whole(far_y), i + 2)

        return begin, forward, last

    def gather_own(b):
        t = ring(cx, off[b], nx)
        part = lambda s, n: lambda y: hf_a.at[0, pl.ds(s, n), t, y]
        return gather("own", sem("own", 3 * b), part(0, SUB), part(0, SUB // 2), part(SUB // 2, SUB // 2))

    def gather_a(g):
        part = lambda s, n: lambda y: hf_a.at[pl.ds(1, nx - 1), pl.ds(g * batch + s, n), :, y]
        return gather("aga", sem("aga", 3 * g), part(0, batch), part(0, batch // 2), part(batch // 2, batch // 2))

    def gather_b(s):
        part = lambda c, n: lambda y: hf_b.at[pl.ds(c, n), s, :, y]
        return gather("agb", sem("agb", 3 * s), part(0, nx), part(0, nx // 2), part(nx // 2, nx // 2))

    own_gathers = [gather_own(b) for b in range(nx)]
    a_gathers = [gather_a(g) for g in range(GROUPS)]
    b_gathers = [gather_b(s) for s in range(SUB)]

    def own_a(b):
        own_gathers[b][0]()

    def own_a_forward(b):
        own_gathers[b][1]()

    def own_a_last(b):
        own_gathers[b][2]()

    def ag_a(g):
        got(hst_a.at[pl.ds(0, nx - 1), pl.ds(0, batch)], sem("h2a", g))
        a_gathers[g][0]()

    def ag_a_forward(g):
        a_gathers[g][1]()

    def ag_a_last(g):
        a_gathers[g][2]()

    def ag_b(s):
        got(hst_b.at[pl.ds(0, nx - 1), 0], sem("h2b", s))
        b_gathers[s][0]()

    def ag_b_forward(s):
        b_gathers[s][1]()

    def ag_b_last(s):
        b_gathers[s][2]()

    ew, lw = early * tw, LATE * tw
    npt = 2 * krows // ew
    steps = dloc // (npt * tw)
    kept = lw // tok

    def rows_of(c, skip, count, use):
        at = pl.ds(pl.multiple_of(lax.rem(c, 2) * (ew + lw) + skip, 128), count)

        @pl.when(c // 2 == k)
        def _():
            use(wout, at)

        @pl.when(c // 2 != k)
        def _():
            use(wo_hbm, at)

    def we_load(i, slot):
        for j in range(npt):
            for p in range(nx):
                cols = pl.ds(pl.multiple_of((i * npt + j) * tw, 128), tw)
                dst = wt.at[slot, p, pl.ds(j * ew, ew)]
                rows_of(ring(cx, p, nx), 0, ew, lambda ref, at: pltpu.make_async_copy(ref.at[at, cols], dst, ls.at[1 + slot]).start())

    def we_wait(slot):
        ref = wt.at[slot, :, pl.ds(0, npt * ew)]
        pltpu.make_async_copy(ref, ref, ls.at[1 + slot]).wait()

    def down_early_load():
        for i in range(min(2, steps)):
            we_load(i, i)

    def down_early(g, loaded=False):
        some = pl.ds(g * batch, batch)
        if not loaded:
            down_early_load()

        def step(i, _):
            slot = lax.rem(i, 3)
            we_wait(slot)

            @pl.when(i + 2 < steps)
            def _():
                we_load(i + 2, lax.rem(i + 2, 3))

            for j in range(npt):
                v = None
                for p in range(nx):
                    h = hf_a[p, some].reshape(batch * nx * sub, ew)
                    w = jnp.dot(h, wt[slot, p, pl.ds(j * ew, ew)], preferred_element_type=jnp.float32)
                    v = w if v is None else v + w
                cols = pl.ds(pl.multiple_of((i * npt + j) * tw, 128), tw)
                acc[some, :, :, cols] = v.reshape(batch, nx, sub, tw)
            return 0

        lax.fori_loop(0, steps, step, 0)

    def late_start():
        drain("zf", z.at[0, pl.ds(0, 2)])
        drain("zy", z.at[pl.ds(0, nx - 1), pl.ds(0, ny - 1)])
        for p in range(nx):
            for j in range(kept):
                rows_of(ring(cx, p, nx), ew + j * tok, tok, lambda ref, at: pltpu.make_async_copy(ref.at[at], z.at[p, j], ls.at[4]).start())

    def late_wait():
        ref = z.at[:, pl.ds(0, kept)]
        pltpu.make_async_copy(ref, ref, ls.at[4]).wait()

    def down_late(s):
        wide = 2 * tw

        def step(i, _):
            cols = pl.ds(pl.multiple_of(i * wide, 128), wide)
            v = None
            for c in range(nx):
                h = hf_b[c, s].reshape(nx * sub, lw)
                p = jnp.dot(h, z[c, pl.ds(0, kept), :, cols].reshape(lw, wide), preferred_element_type=jnp.float32)
                v = p if v is None else v + p
            acc[s, :, :, cols] += v.reshape(nx, sub, wide)
            return 0

        lax.fori_loop(0, dloc // wide, step, 0)

    top, low = pl.ds(0, sub // 2), pl.ds(sub // 2, sub // 2)
    right, left, across = ring(cx, 1, nx), ring(cx, -1, nx), ring(cx, 2, nx)

    def y_send(s):
        send(acc.at[s, across, top], ya.at[s, 0], dev(dx=1), sem("y", 3 * s), "y")
        send(acc.at[s, across, low], ya.at[s, 1], dev(dx=-1), sem("y", 3 * s + 1), "y")
        send(acc.at[s, right, low], yb.at[s, 0, low], dev(dx=1), sem("y", 3 * s + 2), "y")
        send(acc.at[s, left, top], yb.at[s, 1, top], dev(dx=-1), sem("y", 3 * s + 2), "y")

    def y_forward(s):
        got(ya.at[s, 0], sem("y", 3 * s))
        acc[s, right, top] += ya[s, 0]
        send(acc.at[s, right, top], yb.at[s, 0, top], dev(dx=1), sem("y", 3 * s + 2), "y")
        got(ya.at[s, 1], sem("y", 3 * s + 1))
        acc[s, left, low] += ya[s, 1]
        send(acc.at[s, left, low], yb.at[s, 1, low], dev(dx=-1), sem("y", 3 * s + 2), "y")

    def y_final(s):
        got(yb.at[s], sem("y", 3 * s + 2))
        for c in range(ny):
            rows, at = pl.ds(c * piece, piece), pl.ds(c * (tok // ny) + s * piece, piece)
            total = acc[s, cx, rows] + (yb[s, 0, rows] + yb[s, 1, rows])
            ov[at, :] = (xv[at, :].astype(jnp.float32) + total).astype(ov.dtype)

    n0, n1, n2, n3, n4, n5, n6, n7 = range(8)
    yes = True
    zy_own_near()
    zx_forward()
    w_issue(n1)
    w_issue(n2)
    zy_forward(n2)
    zx_last()
    zy_send(n3)
    w_issue(n3)
    w_issue(n4)
    zy_last(n0)
    w_forward(n0)
    w_forward(n1)
    zy_own_rest()
    w_ready(n1)
    up(n0, n1, n2, n0, n1)
    zy_forward(n1)
    zy_forward(n3)
    w_forward(n2)
    w_ready(n2)
    up(n0, n2, n3, n0, n1)
    zy_last(n2)
    w_forward(n3)
    zy_last(n1)
    w_ready(n0)
    up(n0, n0, n3, n2, n3)
    w_ready(n3)
    up(n0, n3, n4, n0, n3)
    up_load(n0, n4)
    h1_a(n2)
    zy_last(n3)
    up(n0, n0, n4, n3, n4, yes)
    up_load(n0, n1)
    h1_a(n3)
    h1_wait(n2)
    w_issue(n5)
    own_a(n2)
    up(n0, n0, n1, n0, n1, yes)
    up_load(n0, n3)
    h1_a(n0)
    h1_wait(n3)
    h2_a(n2, n0)
    up(n0, n0, n3, n1, n2, yes)
    h1_a(n1)
    h2_a(n3, n0)
    h1_wait(n0)
    h2_a(n0, n0)
    h2_a(n0, n1)
    own_a(n3)
    h1_wait(n1)
    own_a(n1)
    h2_a(n1, n0)
    h2_a(n2, n1)
    w_forward(n4)
    own_a(n0)
    h2_a(n2, n2)
    h2_a(n0, n2)
    own_a_forward(n2)
    own_a_forward(n3)
    own_a_forward(n1)
    own_a_last(n3)
    own_a_forward(n0)
    w_forward(n5)
    ag_a(n0)
    h2_a(n1, n1)
    h2_a(n3, n1)
    h2_a(n3, n2)
    h2_a(n1, n2)
    w_issue(n6)
    w_ready(n4)
    up(n1, n4, n5, n0, n4)
    own_a_last(n2)
    ag_a(n1)
    w_ready(n5)
    up(n1, n5, n6, n0, n4)
    ag_a(n2)
    got(wo_hbm, sem("wout"))
    ag_a_forward(n0)
    w_forward_near(n6)
    ag_a_forward(n1)
    up_near(n6)
    ag_a_forward(n2)
    w_forward_far(n6)
    up_far(n6)
    down_early_load()
    h1_b(n0)
    h1_b(n1)
    h1_b(n2)
    h1_b(n3)
    h1_b(n4)
    ag_a_last(n0)
    h1_b(n5)
    late_start()
    ag_a_last(n1)
    own_a_last(n0)
    h2_b(n0)
    own_a_last(n1)
    down_early(n0, yes)
    down_early_load()
    h2_a(n2, n3)
    h2_a(n0, n3)
    ag_b(n0)
    h2_b(n1)
    h2_a(n1, n3)
    h2_b(n2)
    h2_b(n3)
    h1_b(n6)
    h1_b(n7)
    down_early(n1, yes)
    down_early_load()
    h2_b(n4)
    ag_b_forward(n0)
    late_wait()
    ag_b(n1)
    h2_a(n3, n3)
    h2_b(n5)
    ag_b(n2)
    h2_b(n6)
    h2_b(n7)
    ag_b_last(n0)
    down_late(n0)
    y_send(n0)
    ag_b_forward(n1)
    ag_b(n3)
    ag_a_last(n2)
    down_early(n2, yes)
    down_early_load()
    ag_b_forward(n2)
    ag_b(n4)
    y_forward(n0)
    ag_b_last(n1)
    ag_b(n5)
    down_late(n1)
    y_send(n1)
    y_forward(n1)
    ag_b_last(n2)
    down_late(n2)
    ag_b_forward(n3)
    y_send(n2)
    ag_b_forward(n4)
    ag_b_forward(n5)
    ag_a(n3)
    y_forward(n2)
    ag_b_last(n3)
    down_late(n3)
    y_send(n3)
    ag_b_last(n4)
    down_late(n4)
    ag_b_last(n5)
    y_send(n4)
    y_final(n0)
    ag_b(n6)
    down_late(n5)
    ag_a_forward(n3)
    y_send(n5)
    ag_b_forward(n6)
    y_forward(n4)
    ag_b(n7)
    y_forward(n5)
    y_forward(n3)
    ag_a_last(n3)
    down_early(n3, yes)
    ag_b_last(n6)
    down_late(n6)
    y_send(n6)
    ag_b_forward(n7)
    y_final(n2)
    y_final(n1)
    y_forward(n6)
    ag_b_last(n7)
    down_late(n7)
    y_send(n7)
    y_final(n3)
    y_final(n4)
    y_final(n6)
    y_forward(n7)
    y_final(n5)
    y_final(n7)
    three = pl.ds(0, nx - 1)
    drain("stat", stat.at[three])
    drain("gain", gains.at[three])
    drain("mean", means.at[pl.ds(0, 2)])
    drain("raw", z.at[0])
    drain("w", w_hbm.at[:, three])
    drain("pair", w_hbm.at[:, pl.ds(0, nx)])
    drain("wout", wo_hbm)
    for kind in ("h1a", "h2a", "own"):
        drain(kind, hst_a.at[three])
    for kind in ("h1b", "h2b"):
        drain(kind, hst_b.at[three])
    drain("aga", hf_a.at[three, :, :, three])
    drain("agb", hf_b.at[:, :, :, three])
    drain("y", acc.at[:, three])


def solution(mesh):
    nx, ny = mesh.shape["row"] // 2, mesh.shape["col"]

    def local_block(x, gain, win, wout):
        tok, dloc = x.shape
        krows, floc = win.shape
        width = floc // nx
        tw = width // 7
        tiles = width // tw
        early = tiles - LATE
        ew, lw = early * tw, LATE * tw
        sub = tok // SUB
        piece = sub // ny
        bf, f32 = jnp.bfloat16, jnp.float32
        count = plan(tiles).total
        hbm = lambda shape, dt: jax.ShapeDtypeStruct(shape, dt)
        outs = pl.pallas_call(
            functools.partial(block, (nx, ny, dloc * ny)),
            name="mlp_block",
            out_shape=[
                pltpu.VMEM((tok, dloc), bf),
                hbm((tiles, 2 * nx, krows, tw), bf),
                hbm(wout.shape, bf),
                hbm((ny, SUB, nx, piece, ew), bf),
                hbm((ny, SUB, nx, piece, lw), bf),
            ],
            in_specs=[
                pl.BlockSpec(memory_space=pl.ANY),
                pl.BlockSpec(memory_space=pltpu.VMEM),
                pl.BlockSpec(memory_space=pl.ANY),
                pl.BlockSpec(memory_space=pl.ANY),
            ],
            out_specs=[pl.BlockSpec(memory_space=pltpu.VMEM)] + [pl.BlockSpec(memory_space=pl.ANY)] * 4,
            scratch_shapes=[
                pltpu.VMEM((tok, dloc), bf),
                pltpu.VMEM((3, tok, 128), f32),
                pltpu.VMEM((ny, 8, tok), f32),
                pltpu.VMEM((3, 8, tok), f32),
                pltpu.VMEM((ny, 1, dloc), f32),
                pltpu.VMEM((nx, ny, tok, dloc), bf),
                pltpu.VMEM((3, ny, 2 * krows, tw), bf),
                pltpu.VMEM((nx, ny, SUB, piece, ew), bf),
                pltpu.VMEM((nx, ny, SUB, piece, lw), bf),
                pltpu.VMEM((nx, SUB, nx, ny, piece, ew), bf),
                pltpu.VMEM((nx, SUB, nx, ny, piece, lw), bf),
                pltpu.VMEM((SUB, nx, sub, dloc), f32),
                pltpu.VMEM((nx, tok, tw), f32),
                pltpu.VMEM((SUB, 2, sub // 2, dloc), f32),
                pltpu.VMEM((SUB, 2, sub, dloc), f32),
                pltpu.SemaphoreType.DMA((len(KINDS),)),
                pltpu.SemaphoreType.DMA((count,)),
                pltpu.SemaphoreType.DMA((5,)),
            ],
            compiler_params=pltpu.CompilerParams(
                collective_id=0, has_side_effects=True, vmem_limit_bytes=65900000
            ),
        )(x, gain.reshape(1, dloc), win, wout)
        return outs[0]

    return jax.shard_map(
        local_block,
        mesh=mesh,
        in_specs=(P(("dp", "row"), "col"), P("col"), P("row", "col"), P("row", "col")),
        out_specs=P(("dp", "row"), "col"),
        check_vma=False,
    )
```

```python
import functools

import jax
import jax.numpy as jnp
from jax import lax
from jax.experimental import pallas as pl
from jax.experimental.pallas import tpu as pltpu
from jax.sharding import PartitionSpec as P

NORM_EPS = 1e-5
MESH = pl.DeviceIdType.MESH
NEAR_FIRST = (1, 3, 2)
SUB = 8
GROUPS = 4
MID, LATE = 2, 2


def gelu(v):
    return 0.5 * v * (1.0 + jnp.tanh(0.7978845608028654 * (v + 0.044715 * (v * v * v))))


KINDS = (
    "stat", "gain", "mean", "raw", "zf", "zy", "w", "pair", "wout", "h1a", "h2a", "h1b", "h2b", "own", "aga", "h1m", "h2m", "agm", "agb", "y",
)


class Sems:
    def __init__(self):
        self.base, self.total = {}, 0

    def add(self, name, count):
        self.base[name] = self.total
        self.total += count

    def __call__(self, name, index=0):
        return self.base[name] + index


def plan(tiles):
    s = Sems()
    for name, count in (
        ("stat", 1), ("gain", 1), ("mean", 2), ("zx", 4), ("zy", 16), ("rest", 4), ("w", 3 * tiles), ("wf", tiles + 1),
        ("wout", 1), ("h1a", 4), ("h1m", SUB), ("h1b", SUB), ("h2a", GROUPS), ("h2m", SUB), ("h2b", SUB),
        ("own", 12), ("aga", 3 * GROUPS), ("agm", 3 * SUB), ("agb", 3 * SUB), ("y", 3 * SUB),
    ):
        s.add(name, count)
    return s


def block(n, x_hbm, gain_ref, win, wout, ov, w_hbm, wo_hbm, hst_a, hst_m, hst_b,
          xv, sums, stat, means, gains, z, wt, hm_a, hm_m, hm_b, hf_a, hf_m, hf_b, acc, pre, ya, yb, ss, rs, ls):
    nx, ny, d_model = n
    row, cy = lax.axis_index("row"), lax.axis_index("col")
    cx, k = row // 2, lax.rem(row, 2)
    tok, dloc = ov.shape
    tiles, krows, tw = w_hbm.shape[0], w_hbm.shape[2], w_hbm.shape[3]
    early = tiles - MID - LATE
    half = tok // 2
    sub = tok // SUB
    piece = sub // ny
    batch = SUB // GROUPS
    sem = plan(tiles)

    def ring(v, d, m):
        return lax.rem(v + (d + m), m)

    def dev(dx=0, dy=0, core=None):
        return {"row": 2 * ring(cx, dx, nx) + (k if core is None else core), "col": ring(cy, dy, ny)}

    partner = dev(core=1 - k)

    def remote(src, dst, where, i, kind):
        return pltpu.make_async_remote_copy(
            src_ref=src, dst_ref=dst, send_sem=ss.at[KINDS.index(kind)], recv_sem=rs.at[i], device_id=where, device_id_type=MESH
        )

    def send(src, dst, where, i, kind):
        remote(src, dst, where, i, kind).start()

    def got(ref, i):
        remote(ref, ref, partner, i, "w").wait_recv()

    def drain(kind, ref):
        remote(ref, ref, partner, 0, kind).wait_send()

    barrier = pltpu.get_barrier_semaphore()
    peers = [partner] + [dev(dx=d) for d in range(1, nx)] + [dev(dy=d) for d in range(1, ny)]
    for p in peers:
        pl.semaphore_signal(barrier, inc=1, device_id=p, device_id_type=MESH)
    load_x = pltpu.make_async_copy(x_hbm, xv, ls.at[0])
    load_x.start()
    pl.semaphore_wait(barrier, len(peers))

    off = (0, 1, 3, 2)
    lo, hi = pl.ds(0, half), pl.ds(half, half)

    def zb(b, dy, rows=None):
        ref = z.at[ring(cx, off[b], nx), ring(cy, dy, ny)]
        return ref if rows is None else ref.at[rows]

    def raw(rows, where, i):
        send(x_hbm.at[rows], zb(0, 0, rows), where, i, "raw")

    raw(lo, dev(dy=1), sem("zy", 0))
    raw(hi, dev(dy=-1), sem("zy", 1))
    raw(lo, dev(dx=1), sem("zx", 0))
    raw(hi, dev(dx=-1), sem("zx", 1))
    load_x.wait()

    lane = lax.broadcasted_iota(jnp.int32, (32, sums.shape[2]), 1)

    def part(i, _):
        at = pl.ds(pl.multiple_of(i * 32, 32), 32)
        v = xv[at, :].astype(jnp.float32)
        s1 = jnp.sum(v, axis=1, keepdims=True)
        s2 = jnp.sum(v * v, axis=1, keepdims=True)
        sums[0, at, :] = jnp.where(lane == 0, s1, s2)
        return 0

    lax.fori_loop(0, tok // 32, part, 0)
    stat[cy] = jnp.transpose(sums[0])[: stat.shape[1]]
    gains[cy] = gain_ref[...]
    for d in NEAR_FIRST:
        send(stat.at[cy], stat.at[cy], dev(dy=d), sem("stat"), "stat")
    for d in NEAR_FIRST:
        send(gains.at[cy], gains.at[cy], dev(dy=d), sem("gain"), "gain")
    raw(hi, dev(dy=1), sem("rest", 0))
    raw(lo, dev(dy=-1), sem("rest", 1))
    raw(hi, dev(dx=1), sem("rest", 2))
    raw(lo, dev(dx=-1), sem("rest", 3))

    def columns(dx, t):
        return pl.ds(pl.multiple_of(ring(cx, dx, nx) * (tiles * tw) + t * tw, 128), tw)

    last = tiles - 1

    def w_issue(t):
        for d in NEAR_FIRST:
            send(win.at[:, columns(d, t)], w_hbm.at[t, row], dev(dx=d), sem("w", 3 * t + d - 1), "w")
        send(win.at[:, columns(0, t)], w_hbm.at[t, row], partner, sem("wf", t), "pair")

    def w_pass(t, ds):
        for d in ds:
            slot = 2 * ring(cx, -d, nx) + k
            got(w_hbm.at[t, slot], sem("w", 3 * t + d - 1))
            i = sem("wf", tiles if t == last and d == NEAR_FIRST[-1] else t)
            send(w_hbm.at[t, slot], w_hbm.at[t, slot], partner, i, "pair")

    def w_forward(t):
        w_pass(t, NEAR_FIRST)

    def w_ready(t):
        got(w_hbm.at[t, pl.ds(0, nx)], sem("wf", t))

    def w_forward_near(t):
        w_pass(t, NEAR_FIRST[:-1])

    def w_forward_far(t):
        w_pass(t, NEAR_FIRST[-1:])

    got(stat.at[pl.ds(0, ny - 1)], sem("stat"))
    total = (stat[0] + stat[1]) + (stat[2] + stat[3])
    mean = total[0:1] / d_model
    rstd = lax.rsqrt(total[1:2] / d_model - mean * mean + NORM_EPS)
    means[0] = jnp.where(lax.broadcasted_iota(jnp.int32, total.shape, 0) == 0, mean, rstd)
    send(means.at[0], means.at[2], dev(dx=1), sem("mean", 0), "mean")
    send(means.at[0], means.at[1], dev(dx=-1), sem("mean", 1), "mean")
    w_issue(0)
    send(wout, wo_hbm, partner, sem("wout"), "wout")

    def spread(b):
        copies = sums.shape[2] // means.shape[1]
        sums[b] = jnp.transpose(jnp.concatenate([means[b]] * copies, axis=0))

    def normalise(b, y, src=None, r0=0, r1=tok):
        t = ring(cx, off[b], nx)

        def norm(i, _):
            at = pl.ds(pl.multiple_of(i * 32, 32), 32)
            v = (z[t, y, at, :] if src is None else src[at, :]).astype(jnp.float32)
            z[t, y, at, :] = ((v - sums[b, at, 0:1]) * sums[b, at, 1:2] * gains[y]).astype(z.dtype)
            return 0

        lax.fori_loop(r0 // 32, r1 // 32, norm, 0)

    spread(0)
    normalise(0, cy, xv)

    up_y, down_y, far_y = ring(cy, 1, ny), ring(cy, -1, ny), ring(cy, 2, ny)

    def zx_forward():
        got(zb(2, 0, lo), sem("zx", 0))
        got(means.at[0], sem("mean", 0))
        got(zb(2, 0, hi), sem("rest", 2))
        spread(2)
        normalise(2, cy)
        send(zb(2, 0, lo), zb(2, 0, lo), dev(dx=1), sem("zx", 2), "zf")
        zy_send(2)
        got(zb(1, 0, hi), sem("zx", 1))
        got(means.at[0], sem("mean", 1))
        got(zb(1, 0, lo), sem("rest", 3))
        spread(1)
        normalise(1, cy)
        send(zb(1, 0, hi), zb(1, 0, hi), dev(dx=-1), sem("zx", 3), "zf")
        zy_send(1)

    def zx_last():
        got(zb(3, 0, lo), sem("zx", 2))
        got(zb(3, 0, hi), sem("zx", 3))

    def zy_send(b):
        send(zb(b, 0), zb(b, 0), dev(dy=1), sem("zy", 4 * b), "zy")
        send(zb(b, 0), zb(b, 0), dev(dy=-1), sem("zy", 4 * b + 1), "zy")

    def zy_forward(b):
        got(zb(b, -1), sem("zy", 4 * b))
        send(zb(b, -1, lo), zb(b, -1, lo), dev(dy=1), sem("zy", 4 * b + 2), "zy")
        got(zb(b, 1), sem("zy", 4 * b + 1))
        send(zb(b, 1, hi), zb(b, 1, hi), dev(dy=-1), sem("zy", 4 * b + 3), "zy")

    def zy_last(b):
        got(zb(b, 2, lo), sem("zy", 4 * b + 2))
        got(zb(b, 2, hi), sem("zy", 4 * b + 3))

    def zy_own_near():
        got(gains.at[pl.ds(0, ny - 1)], sem("gain"))
        got(zb(0, -1, lo), sem("zy", 0))
        normalise(0, down_y, None, 0, half)
        send(zb(0, -1, lo), zb(0, -1, lo), dev(dy=1), sem("zy", 2), "zf")
        got(zb(0, 1, hi), sem("zy", 1))
        normalise(0, up_y, None, half, tok)
        send(zb(0, 1, hi), zb(0, 1, hi), dev(dy=-1), sem("zy", 3), "zf")

    def zy_own_rest():
        got(zb(0, -1, hi), sem("rest", 0))
        normalise(0, down_y, None, half, tok)
        got(zb(0, 1, lo), sem("rest", 1))
        normalise(0, up_y, None, 0, half)

    def wt_rows(t, slot, rows):
        for j in rows:
            for core in range(2):
                r = 2 * ring(cx, j, nx) + lax.rem(k + core, 2)
                dst = wt.at[slot, r // 2, pl.ds(pl.multiple_of(lax.rem(r, 2) * krows, krows), krows)]
                src = win.at[:, columns(0, t)] if j == 0 and core == 0 else w_hbm.at[t, r]
                pltpu.make_async_copy(src, dst, ls.at[1 + slot]).start()

    def wt_load(t, slot):
        wt_rows(t, slot, range(nx))

    def wt_wait(slot):
        pltpu.make_async_copy(wt.at[slot], wt.at[slot], ls.at[1 + slot]).wait()

    def up_load(t0, t1):
        for i in range(min(2, t1 - t0)):
            wt_load(t0 + i, i)

    def up(part, t0, t1, b0, b1, loaded=False):
        hm, hf, first = ((hm_a, hf_a, 0), (hm_m, hf_m, early), (hm_b, hf_b, early + MID))[part]
        if not loaded:
            up_load(t0, t1)

        def tile(i, _):
            slot = lax.rem(i, 3)
            wt_wait(slot)

            @pl.when(i + 2 < t1 - t0)
            def _():
                wt_load(t0 + i + 2, lax.rem(i + 2, 3))

            at = pl.ds(pl.multiple_of((t0 + i - first) * tw, 128), tw)

            def rows(b, _):
                t = ring(cx, b + b // 2 - 2 * (b // 3), nx)
                v = jnp.dot(z[t, 0], wt[slot, 0], preferred_element_type=jnp.float32)
                for j in range(1, ny):
                    v += jnp.dot(z[t, j], wt[slot, j], preferred_element_type=jnp.float32)
                hm[t, :, :, :, at] = gelu(v).astype(hm.dtype).reshape(ny, SUB, piece, tw)

                @pl.when(cx == cy)
                def _():
                    hf[0, :, t, cy, :, at] = hm[t, cy, :, :, at]

                return 0

            lax.fori_loop(b0, b1, rows, 0)
            return 0

        lax.fori_loop(0, t1 - t0, tile, 0)

    def up_near(t):
        got(w_hbm.at[t, pl.ds(0, nx - 1)], sem("wf", t))
        wt_rows(t, 0, (0, 1, 3))
        ref = wt.at[0, pl.ds(0, ny - 1)]
        pltpu.make_async_copy(ref, ref, ls.at[1]).wait()

        def rows(b, _):
            v = None
            for j in (0, 1, 3):
                f = ring(cx, j, nx)
                p = jnp.dot(z[b, f], wt[0, f], preferred_element_type=jnp.float32)
                v = p if v is None else v + p
            pre[b] = v
            return 0

        lax.fori_loop(0, nx, rows, 0)

    def up_far(t):
        got(w_hbm.at[t, row], sem("wf", tiles))
        wt_rows(t, 0, (2,))
        f = ring(cx, 2, nx)
        pltpu.make_async_copy(wt.at[0, f], wt.at[0, f], ls.at[1]).wait()
        at = pl.ds((t - early - MID) * tw, tw)

        def rows(b, _):
            v = pre[b] + jnp.dot(z[b, f], wt[0, f], preferred_element_type=jnp.float32)
            hm_b[b, :, :, :, at] = gelu(v).astype(hm_b.dtype).reshape(ny, SUB, piece, tw)

            @pl.when(cx == cy)
            def _():
                hf_b[0, :, b, cy, :, at] = hm_b[b, cy, :, :, at]

            return 0

        lax.fori_loop(0, nx, rows, 0)

    def h1_a(b):
        t = ring(cx, off[b], nx)
        for d in NEAR_FIRST:
            c = ring(cy, d, ny)
            i = sem("h1a", b)

            @pl.when(cx == cy)
            def _():
                remote(hm_a.at[t, c], hf_a.at[0, :, t, c], dev(dy=d), i, "h1a").start()

            @pl.when(cx != cy)
            def _():
                remote(hm_a.at[t, c], hst_a.at[cy, :, t], dev(dy=d), i, "h1a").start()

    def h1_wait(b):
        got(hst_a.at[pl.ds(0, ny - 1), :, 0], sem("h1a", b))

    def h2_a(b, g):
        t = ring(cx, off[b], nx)
        some = pl.ds(g * batch, batch)
        for d in NEAR_FIRST:
            c = ring(cx, d, nx)
            i = sem("h2a", g)

            @pl.when(c == cy)
            def _():
                remote(hm_a.at[t, cy, some], hf_a.at[nx - d, some, t, cy], dev(dx=d), i, "h2a").start()

            @pl.when(c != cy)
            def _():
                remote(hst_a.at[c, some, t], hf_a.at[nx - d, some, t, cy], dev(dx=d), i, "h2a").start()

    def spread_h(kind, hm, hst, hf):
        def h1(s):
            for d in NEAR_FIRST:
                c = ring(cy, d, ny)
                i = sem("h1" + kind, s)

                @pl.when(cx == cy)
                def _():
                    remote(hm.at[:, c, s], hf.at[0, s, :, c], dev(dy=d), i, "h1" + kind).start()

                @pl.when(cx != cy)
                def _():
                    remote(hm.at[:, c, s], hst.at[cy, s], dev(dy=d), i, "h1" + kind).start()

        def h2(s):
            got(hst.at[pl.ds(0, ny - 1), 0], sem("h1" + kind, s))
            for d in NEAR_FIRST:
                c = ring(cx, d, nx)
                i = sem("h2" + kind, s)

                @pl.when(c == cy)
                def _():
                    remote(hm.at[:, cy, s], hf.at[nx - d, s, :, cy], dev(dx=d), i, "h2" + kind).start()

                @pl.when(c != cy)
                def _():
                    remote(hst.at[c, s], hf.at[nx - d, s, :, cy], dev(dx=d), i, "h2" + kind).start()

        return h1, h2

    h1_m, h2_m = spread_h("m", hm_m, hst_m, hf_m)
    h1_b, h2_b = spread_h("b", hm_b, hst_b, hf_b)

    def gather(kind, i, whole, low, high):
        def begin():
            send(whole(cy), whole(cy), dev(dy=1), i, kind)
            send(whole(cy), whole(cy), dev(dy=-1), i + 1, kind)

        def forward():
            got(whole(cy), i)
            send(low(down_y), low(down_y), dev(dy=1), i + 2, kind)
            got(whole(cy), i + 1)
            send(high(up_y), high(up_y), dev(dy=-1), i + 2, kind)

        def last():
            got(whole(far_y), i + 2)

        return begin, forward, last

    def gather_own(b):
        t = ring(cx, off[b], nx)
        part = lambda s, n: lambda y: hf_a.at[0, pl.ds(s, n), t, y]
        return gather("own", sem("own", 3 * b), part(0, SUB), part(0, SUB // 2), part(SUB // 2, SUB // 2))

    def gather_a(g):
        part = lambda s, n: lambda y: hf_a.at[pl.ds(1, nx - 1), pl.ds(g * batch + s, n), :, y]
        return gather("aga", sem("aga", 3 * g), part(0, batch), part(0, batch // 2), part(batch // 2, batch // 2))

    def gather_late(kind, s, hst, hf):
        part = lambda c, n: lambda y: hf.at[pl.ds(c, n), s, :, y]
        begin, forward, last = gather("ag" + kind, sem("ag" + kind, 3 * s), part(0, nx), part(0, nx // 2), part(nx // 2, nx // 2))

        def start():
            got(hst.at[pl.ds(0, nx - 1), 0], sem("h2" + kind, s))
            begin()

        return start, forward, last

    own_gathers = [gather_own(b) for b in range(nx)]
    a_gathers = [gather_a(g) for g in range(GROUPS)]
    m_gathers = [gather_late("m", s, hst_m, hf_m) for s in range(SUB)]
    b_gathers = [gather_late("b", s, hst_b, hf_b) for s in range(SUB)]

    def own_a(b):
        own_gathers[b][0]()

    def own_a_forward(b):
        own_gathers[b][1]()

    def own_a_last(b):
        own_gathers[b][2]()

    def ag_a(g):
        got(hst_a.at[pl.ds(0, nx - 1), pl.ds(0, batch)], sem("h2a", g))
        a_gathers[g][0]()

    def ag_a_forward(g):
        a_gathers[g][1]()

    def ag_a_last(g):
        a_gathers[g][2]()

    def ag_m(s):
        m_gathers[s][0]()

    def ag_m_forward(s):
        m_gathers[s][1]()

    def ag_m_last(s):
        m_gathers[s][2]()

    def ag_b(s):
        b_gathers[s][0]()

    def ag_b_forward(s):
        b_gathers[s][1]()

    def ag_b_last(s):
        b_gathers[s][2]()

    ew, mw, lw = early * tw, MID * tw, LATE * tw
    npt = 2 * krows // ew
    steps = dloc // (npt * tw)
    kept, kept_m = (mw + lw) // tok, mw // tok

    def rows_of(c, skip, count, use):
        at = pl.ds(pl.multiple_of(lax.rem(c, 2) * (ew + mw + lw) + skip, 128), count)

        @pl.when(c // 2 == k)
        def _():
            use(wout, at)

        @pl.when(c // 2 != k)
        def _():
            use(wo_hbm, at)

    def we_load(i, slot):
        for j in range(npt):
            for p in range(nx):
                cols = pl.ds(pl.multiple_of((i * npt + j) * tw, 128), tw)
                dst = wt.at[slot, p, pl.ds(j * ew, ew)]
                rows_of(ring(cx, p, nx), 0, ew, lambda ref, at: pltpu.make_async_copy(ref.at[at, cols], dst, ls.at[1 + slot]).start())

    def we_wait(slot):
        ref = wt.at[slot, :, pl.ds(0, npt * ew)]
        pltpu.make_async_copy(ref, ref, ls.at[1 + slot]).wait()

    def down_early_load():
        for i in range(min(2, steps)):
            we_load(i, i)

    def down_early(g, loaded=False):
        some = pl.ds(g * batch, batch)
        if not loaded:
            down_early_load()

        def step(i, _):
            slot = lax.rem(i, 3)
            we_wait(slot)

            @pl.when(i + 2 < steps)
            def _():
                we_load(i + 2, lax.rem(i + 2, 3))

            for j in range(npt):
                v = None
                for p in range(nx):
                    h = hf_a[p, some].reshape(batch * nx * sub, ew)
                    w = jnp.dot(h, wt[slot, p, pl.ds(j * ew, ew)], preferred_element_type=jnp.float32)
                    v = w if v is None else v + w
                cols = pl.ds(pl.multiple_of((i * npt + j) * tw, 128), tw)
                acc[some, :, :, cols] = v.reshape(batch, nx, sub, tw)
            return 0

        lax.fori_loop(0, steps, step, 0)

    def late_start():
        drain("zf", z.at[0, pl.ds(0, 2)])
        drain("zy", z.at[pl.ds(0, nx - 1), pl.ds(0, ny - 1)])
        for p in range(nx):
            for j in range(kept):
                rows_of(ring(cx, p, nx), ew + j * tok, tok, lambda ref, at: pltpu.make_async_copy(ref.at[at], z.at[p, j], ls.at[4]).start())

    def late_wait():
        ref = z.at[:, pl.ds(0, kept)]
        pltpu.make_async_copy(ref, ref, ls.at[4]).wait()

    def down_late(s):
        wide = 2 * tw

        def step(i, _):
            cols = pl.ds(pl.multiple_of(i * wide, 128), wide)
            v = None
            for hf, at, depth in ((hf_m, pl.ds(0, kept_m), mw), (hf_b, pl.ds(kept_m, kept - kept_m), lw)):
                for c in range(nx):
                    h = hf[c, s].reshape(nx * sub, depth)
                    p = jnp.dot(h, z[c, at, :, cols].reshape(depth, wide), preferred_element_type=jnp.float32)
                    v = p if v is None else v + p
            acc[s, :, :, cols] += v.reshape(nx, sub, wide)
            return 0

        lax.fori_loop(0, dloc // wide, step, 0)

    top, low = pl.ds(0, sub // 2), pl.ds(sub // 2, sub // 2)
    right, left, across = ring(cx, 1, nx), ring(cx, -1, nx), ring(cx, 2, nx)

    def y_send(s):
        send(acc.at[s, across, top], ya.at[s, 0], dev(dx=1), sem("y", 3 * s), "y")
        send(acc.at[s, across, low], ya.at[s, 1], dev(dx=-1), sem("y", 3 * s + 1), "y")
        send(acc.at[s, right, low], yb.at[s, 0, low], dev(dx=1), sem("y", 3 * s + 2), "y")
        send(acc.at[s, left, top], yb.at[s, 1, top], dev(dx=-1), sem("y", 3 * s + 2), "y")

    def y_forward(s):
        got(ya.at[s, 0], sem("y", 3 * s))
        acc[s, right, top] += ya[s, 0]
        send(acc.at[s, right, top], yb.at[s, 0, top], dev(dx=1), sem("y", 3 * s + 2), "y")
        got(ya.at[s, 1], sem("y", 3 * s + 1))
        acc[s, left, low] += ya[s, 1]
        send(acc.at[s, left, low], yb.at[s, 1, low], dev(dx=-1), sem("y", 3 * s + 2), "y")

    def y_final(s):
        got(yb.at[s], sem("y", 3 * s + 2))
        for c in range(ny):
            rows, at = pl.ds(c * piece, piece), pl.ds(c * (tok // ny) + s * piece, piece)
            total = acc[s, cx, rows] + (yb[s, 0, rows] + yb[s, 1, rows])
            ov[at, :] = (xv[at, :].astype(jnp.float32) + total).astype(ov.dtype)

    n0, n1, n2, n3, n4, n5, n6, n7 = range(8)
    yes = True
    zy_own_near()
    zx_forward()
    w_issue(n1)
    w_issue(n2)
    w_issue(n3)
    w_issue(n4)
    w_issue(n5)
    zy_last(n0)
    zy_own_rest()
    zx_last()
    w_forward(n0)
    zy_forward(n2)
    zy_send(n3)
    w_forward(n1)
    w_ready(n1)
    up(n0, n1, n2, n0, n1)
    zy_forward(n1)
    w_forward(n2)
    zy_forward(n3)
    zy_last(n2)
    w_ready(n0)
    w_ready(n2)
    up(n0, n0, n3, n2, n3)
    up_load(n2, n3)
    h1_a(n2)
    up(n0, n2, n3, n0, n1, yes)
    up(n0, n0, n1, n0, n1)
    up_load(n0, n3)
    h1_a(n0)
    w_forward(n3)
    zy_last(n1)
    up(n0, n0, n3, n1, n2, yes)
    h1_a(n1)
    zy_last(n3)
    w_ready(n3)
    up(n1, n3, n4, n0, n4)
    up_load(n0, n3)
    h1_wait(n0)
    h1_wait(n2)
    own_a(n0)
    own_a(n2)
    w_forward(n4)
    up(n0, n0, n3, n3, n4, yes)
    h1_wait(n1)
    own_a(n1)
    h1_a(n3)
    own_a_forward(n0)
    own_a_forward(n2)
    w_ready(n4)
    up(n1, n4, n5, n0, n4)
    h1_m(n0)
    h1_m(n1)
    h2_a(n0, n0)
    h2_a(n0, n1)
    h2_a(n2, n0)
    h1_m(n2)
    h2_a(n1, n0)
    h1_m(n3)
    h1_m(n4)
    h1_m(n5)
    h1_wait(n3)
    own_a(n3)
    h2_a(n3, n0)
    h2_m(n0)
    h2_a(n1, n1)
    got(wo_hbm, sem("wout"))
    h1_m(n6)
    h1_m(n7)
    w_forward(n5)
    h2_m(n1)
    h2_m(n2)
    h2_a(n2, n1)
    h2_a(n3, n1)
    own_a_forward(n1)
    w_issue(n6)
    ag_a(n0)
    ag_m(n0)
    h2_m(n3)
    h2_m(n4)
    h2_m(n5)
    h2_a(n0, n2)
    h2_a(n3, n2)
    h2_a(n3, n3)
    ag_m(n1)
    ag_a(n1)
    own_a_forward(n3)
    h2_a(n0, n3)
    w_ready(n5)
    up(n2, n5, n6, n0, n4)
    ag_m_forward(n0)
    ag_m_forward(n1)
    h2_a(n1, n2)
    ag_m(n2)
    w_forward_near(n6)
    ag_a_forward(n0)
    ag_a_forward(n1)
    up_near(n6)
    w_forward_far(n6)
    h2_a(n2, n2)
    own_a_last(n0)
    ag_m_last(n0)
    ag_m(n3)
    own_a_last(n1)
    ag_m_forward(n2)
    h2_a(n2, n3)
    ag_m(n4)
    up_far(n6)
    down_early_load()
    h1_b(n0)
    late_start()
    ag_m_last(n1)
    h1_b(n1)
    h2_m(n6)
    h1_b(n2)
    h1_b(n3)
    ag_m_forward(n3)
    own_a_last(n3)
    h1_b(n4)
    h2_b(n0)
    h1_b(n5)
    h1_b(n6)
    h2_b(n1)
    h2_b(n2)
    ag_b(n0)
    ag_b(n1)
    h2_b(n3)
    h2_b(n4)
    own_a_last(n2)
    ag_a_last(n0)
    h2_m(n7)
    ag_a_last(n1)
    ag_m_last(n2)
    ag_b(n2)
    ag_b_forward(n0)
    h2_b(n5)
    ag_b(n3)
    h1_b(n7)
    down_early(n0, yes)
    down_early_load()
    late_wait()
    h2_a(n1, n3)
    ag_b_forward(n1)
    ag_b_forward(n2)
    ag_b(n4)
    ag_a(n2)
    ag_b_last(n0)
    down_late(n0)
    ag_m(n5)
    y_send(n0)
    h2_b(n6)
    h2_b(n7)
    down_early(n1, yes)
    down_early_load()
    ag_b_forward(n3)
    ag_b_last(n2)
    ag_b_last(n1)
    ag_b_forward(n4)
    y_forward(n0)
    down_late(n1)
    y_send(n1)
    ag_m_last(n3)
    ag_a_forward(n2)
    down_late(n2)
    y_final(n0)
    ag_b(n5)
    y_send(n2)
    ag_m_forward(n4)
    ag_m_forward(n5)
    ag_b_last(n3)
    ag_b_last(n4)
    down_late(n3)
    ag_a(n3)
    ag_a_last(n2)
    y_send(n3)
    y_forward(n1)
    ag_b_forward(n5)
    down_early(n2, yes)
    down_early_load()
    ag_b(n6)
    ag_m(n6)
    y_forward(n3)
    ag_m_last(n4)
    down_late(n4)
    ag_a_forward(n3)
    ag_m_last(n5)
    y_send(n4)
    ag_m(n7)
    ag_b_last(n5)
    down_late(n5)
    ag_b_forward(n6)
    y_forward(n2)
    y_send(n5)
    y_forward(n4)
    ag_b(n7)
    ag_a_last(n3)
    ag_m_forward(n6)
    down_early(n3, yes)
    ag_m_forward(n7)
    y_final(n1)
    y_forward(n5)
    ag_b_last(n6)
    ag_b_forward(n7)
    ag_m_last(n6)
    down_late(n6)
    y_send(n6)
    ag_b_last(n7)
    ag_m_last(n7)
    down_late(n7)
    y_send(n7)
    y_final(n5)
    y_final(n2)
    y_forward(n6)
    y_final(n4)
    y_final(n3)
    y_forward(n7)
    y_final(n6)
    y_final(n7)
    three = pl.ds(0, nx - 1)
    drain("stat", stat.at[three])
    drain("gain", gains.at[three])
    drain("mean", means.at[pl.ds(0, 2)])
    drain("raw", z.at[0])
    drain("w", w_hbm.at[:, three])
    drain("pair", w_hbm.at[:, pl.ds(0, nx)])
    drain("wout", wo_hbm)
    for kind in ("h1a", "h2a", "own"):
        drain(kind, hst_a.at[three])
    for part, hst, hf in (("m", hst_m, hf_m), ("b", hst_b, hf_b)):
        drain("h1" + part, hst.at[three])
        drain("h2" + part, hst.at[three])
        drain("ag" + part, hf.at[:, :, :, three])
    drain("aga", hf_a.at[three, :, :, three])
    drain("y", acc.at[:, three])


def solution(mesh):
    nx, ny = mesh.shape["row"] // 2, mesh.shape["col"]

    def local_block(x, gain, win, wout):
        tok, dloc = x.shape
        krows, floc = win.shape
        width = floc // nx
        tw = width // 7
        tiles = width // tw
        early = tiles - MID - LATE
        ew, mw, lw = early * tw, MID * tw, LATE * tw
        sub = tok // SUB
        piece = sub // ny
        bf, f32 = jnp.bfloat16, jnp.float32
        count = plan(tiles).total
        hbm = lambda shape, dt: jax.ShapeDtypeStruct(shape, dt)
        outs = pl.pallas_call(
            functools.partial(block, (nx, ny, dloc * ny)),
            name="mlp_block",
            out_shape=[
                pltpu.VMEM((tok, dloc), bf),
                hbm((tiles, 2 * nx, krows, tw), bf),
                hbm(wout.shape, bf),
                hbm((ny, SUB, nx, piece, ew), bf),
                hbm((ny, SUB, nx, piece, mw), bf),
                hbm((ny, SUB, nx, piece, lw), bf),
            ],
            in_specs=[
                pl.BlockSpec(memory_space=pl.ANY),
                pl.BlockSpec(memory_space=pltpu.VMEM),
                pl.BlockSpec(memory_space=pl.ANY),
                pl.BlockSpec(memory_space=pl.ANY),
            ],
            out_specs=[pl.BlockSpec(memory_space=pltpu.VMEM)] + [pl.BlockSpec(memory_space=pl.ANY)] * 5,
            scratch_shapes=[
                pltpu.VMEM((tok, dloc), bf),
                pltpu.VMEM((3, tok, 128), f32),
                pltpu.VMEM((ny, 8, tok), f32),
                pltpu.VMEM((3, 8, tok), f32),
                pltpu.VMEM((ny, 1, dloc), f32),
                pltpu.VMEM((nx, ny, tok, dloc), bf),
                pltpu.VMEM((3, ny, 2 * krows, tw), bf),
                pltpu.VMEM((nx, ny, SUB, piece, ew), bf),
                pltpu.VMEM((nx, ny, SUB, piece, mw), bf),
                pltpu.VMEM((nx, ny, SUB, piece, lw), bf),
                pltpu.VMEM((nx, SUB, nx, ny, piece, ew), bf),
                pltpu.VMEM((nx, SUB, nx, ny, piece, mw), bf),
                pltpu.VMEM((nx, SUB, nx, ny, piece, lw), bf),
                pltpu.VMEM((SUB, nx, sub, dloc), f32),
                pltpu.VMEM((nx, tok, tw), f32),
                pltpu.VMEM((SUB, 2, sub // 2, dloc), f32),
                pltpu.VMEM((SUB, 2, sub, dloc), f32),
                pltpu.SemaphoreType.DMA((len(KINDS),)),
                pltpu.SemaphoreType.DMA((count,)),
                pltpu.SemaphoreType.DMA((5,)),
            ],
            compiler_params=pltpu.CompilerParams(
                collective_id=0, has_side_effects=True, vmem_limit_bytes=65900000
            ),
        )(x, gain.reshape(1, dloc), win, wout)
        return outs[0]

    return jax.shard_map(
        local_block,
        mesh=mesh,
        in_specs=(P(("dp", "row"), "col"), P("col"), P("row", "col"), P("row", "col")),
        out_specs=P(("dp", "row"), "col"),
        check_vma=False,
    )
```
